128 devices in a mesh: replica: 1, model: 128 (over z, y, x, core).
Axes of the slice: x: 4, y: 4, z: 4, core: 2. Of those that a mesh axis runs over, the one named last changes fastest.
Arguments:
- hidden: bfloat16 [128, 8192], P('replica')
- w_query: bfloat16 [8192, 8192], P(None, 'model')
- w_key: bfloat16 [8192, 64], replicated
- w_value: bfloat16 [8192, 64], replicated
- w_out: bfloat16 [8192, 8192], P('model')
- key_cache: bfloat16 [128, 16384, 64], P(('replica', 'model'))
- value_cache: bfloat16 [128, 16384, 64], P(('replica', 'model'))
- lengths: int32 [128], P('replica')
Outputs:
- output 1: bfloat16 [128, 8192], P('replica')
- output 2: bfloat16 [128, 16384, 64], P(('replica', 'model'))
- output 3: bfloat16 [128, 16384, 64], P(('replica', 'model'))
All inputs are finite; a program needn't handle non-finite values.
Results may differ from the reference program's by a relative error of at most 0.0112356.
Values are sent between devices in bfloat16 or wider.
A program may use at most 1 GiB of HBM per device.

```python
import math
import jax
import jax.numpy as jnp
from jax import lax

MODEL_DIM = 8192
QUERY_HEADS = 128
HEAD_DIM = 64
SEQ_LEN = 16384
BATCH_ROWS = 128
LOG_SEQ = int(math.log2(SEQ_LEN))


def draw_cache_row(row_key):
    return jax.random.normal(row_key, (SEQ_LEN, HEAD_DIM), jnp.float32).astype(jnp.bfloat16)


def draw_lengths(len_keys):
    len_exponent = jax.random.randint(len_keys[0], (BATCH_ROWS,), 0, LOG_SEQ + 1)
    upper_len = jnp.left_shift(jnp.ones_like(len_exponent), len_exponent)
    lower_len = upper_len // 2
    drawn_len = jax.random.randint(len_keys[1], (BATCH_ROWS,), lower_len, upper_len)
    top_row = jax.random.randint(len_keys[2], (), 0, BATCH_ROWS)
    return jnp.where(jnp.arange(BATCH_ROWS) == top_row, SEQ_LEN - 1, drawn_len).astype(jnp.int32)


def setup_inputs(seed: int = 0, part: int = 0) -> dict:
    base_key = jax.random.key(seed)
    shared_keys = jax.random.split(base_key, 4)
    part_keys = jax.random.split(jax.random.fold_in(base_key, part), 6)
    query_width = QUERY_HEADS * HEAD_DIM
    hidden = jax.random.normal(part_keys[0], (BATCH_ROWS, MODEL_DIM), jnp.float32)
    w_query = jax.random.normal(shared_keys[0], (MODEL_DIM, query_width), jnp.float32) * (3.0 / math.sqrt(MODEL_DIM))
    w_key = jax.random.normal(shared_keys[1], (MODEL_DIM, HEAD_DIM), jnp.float32) / math.sqrt(MODEL_DIM)
    w_value = jax.random.normal(shared_keys[2], (MODEL_DIM, HEAD_DIM), jnp.float32) / math.sqrt(MODEL_DIM)
    w_out = jax.random.normal(shared_keys[3], (query_width, MODEL_DIM), jnp.float32) / math.sqrt(query_width)
    key_cache = lax.map(draw_cache_row, jax.random.split(part_keys[1], BATCH_ROWS))
    value_cache = lax.map(draw_cache_row, jax.random.split(part_keys[2], BATCH_ROWS))
    lengths = draw_lengths(part_keys[3:6])
    return {'hidden': hidden.astype(jnp.bfloat16), 'w_query': w_query.astype(jnp.bfloat16), 'w_key': w_key.astype(jnp.bfloat16), 'w_value': w_value.astype(jnp.bfloat16), 'w_out': w_out.astype(jnp.bfloat16), 'key_cache': key_cache, 'value_cache': value_cache, 'lengths': lengths}


def attend_row(row_args):
    query_row, key_row, value_row, row_len = row_args
    scores = jnp.einsum('hd,td->ht', query_row.astype(jnp.float32), key_row.astype(jnp.float32)) * (HEAD_DIM ** -0.5)
    valid_pos = jnp.arange(SEQ_LEN)[None, :] <= row_len
    scores = jnp.where(valid_pos, scores, -jnp.inf)
    weights = jnp.exp(scores - jnp.max(scores, axis=1, keepdims=True))
    weight_sum = jnp.sum(weights, axis=1)
    weighted_sum = jnp.einsum('ht,td->hd', weights.astype(jnp.bfloat16).astype(jnp.float32), value_row.astype(jnp.float32))
    return (weighted_sum / weight_sum[:, None]).astype(jnp.bfloat16)


def reference(hidden, w_query, w_key, w_value, w_out, key_cache, value_cache, lengths):
    query = jnp.dot(hidden, w_query, preferred_element_type=jnp.float32).astype(jnp.bfloat16)
    query = query.reshape(BATCH_ROWS, QUERY_HEADS, HEAD_DIM)
    key_new = jnp.dot(hidden, w_key, preferred_element_type=jnp.float32).astype(jnp.bfloat16)
    value_new = jnp.dot(hidden, w_value, preferred_element_type=jnp.float32).astype(jnp.bfloat16)
    write_pos = jnp.arange(SEQ_LEN)[None, :, None] == lengths[:, None, None]
    key_upd = jnp.where(write_pos, key_new[:, None, :], key_cache)
    value_upd = jnp.where(write_pos, value_new[:, None, :], value_cache)
    context = lax.map(attend_row, (query, key_upd, value_upd, lengths))
    attn_out = jnp.dot(context.reshape(BATCH_ROWS, QUERY_HEADS * HEAD_DIM), w_out, preferred_element_type=jnp.float32)
    hidden_out = (hidden.astype(jnp.float32) + attn_out).astype(jnp.bfloat16)
    return (hidden_out, key_upd, value_upd)
```

```python
import functools
import jax
import jax.numpy as jnp
from jax import lax
from jax.experimental import pallas as pl
from jax.experimental.pallas import tpu as pltpu
from jax.sharding import PartitionSpec as P

F32 = jnp.float32
BF16 = jnp.bfloat16
NT = (((1,), (1,)), ((), ()))
LOG2E = 1.4426950408889634


def dot_nt(lhs, rhs):
    return lax.dot_general(lhs, rhs, NT, preferred_element_type=F32)


def step_kernel(n_dev, x_hbm, wq_hbm, wk_hbm, wv_hbm, wo_hbm, key_hbm, value_hbm, len_ref, out_ref, new_ref,
                x_v, wq_v, wk_v, wv_v, wo_v, key_v, value_v, q_send, q_recv, wo_c, ctx_send, ctx_recv, ctx_wide, ctx_all, out_send,
                load_sem, q_sems, wo_sems, ctx_sems, ctx_in, out_sems, out_in):
    me = lax.axis_index('model')
    core = me % 2
    chip = me // 2
    n_chip = n_dev // 2
    half = me // n_chip
    n_rows, model_dim = x_v.shape
    head_dim, seq_len = key_v.shape
    cols = model_dim // n_chip
    half_rows = n_rows // 2

    def remote(src, dst, send_sem, recv_sem, target):
        return pltpu.make_async_remote_copy(src_ref=src, dst_ref=dst, send_sem=send_sem, recv_sem=recv_sem, device_id={'model': target})

    loads = []
    for n, (src, dst) in enumerate(((x_hbm, x_v), (wq_hbm, wq_v), (wo_hbm, wo_v), (wk_hbm, wk_v), (wv_hbm, wv_v), (key_hbm, key_v), (value_hbm, value_v))):
        copy = pltpu.make_async_copy(src, dst, load_sem.at[n])
        copy.start()
        loads.append(copy)

    barrier = pltpu.get_barrier_semaphore()

    def greet(i, carry):
        pl.semaphore_signal(barrier, inc=1, device_id={'model': (me + i) % n_dev})
        return carry

    lax.fori_loop(1, n_dev, greet, 0)

    loads[0].wait()
    loads[1].wait()
    k_step = 1024

    def project(i, acc):
        at = pl.ds(pl.multiple_of(i * k_step, k_step), k_step)
        return acc + dot_nt(x_v[:, at], wq_v[:, at])

    query = lax.fori_loop(0, model_dim // k_step, project, jnp.zeros((n_rows, head_dim), F32))
    query = query.astype(BF16).astype(F32)
    q_send[:, 0, :] = jnp.concatenate([query, jnp.zeros_like(query)], axis=1)
    slot = core * n_chip + chip
    q_recv[slot] = q_send[me]
    pl.semaphore_wait(barrier, n_dev - 1)

    def send_query(i, carry):
        target = (me + i) % n_dev
        remote(q_send.at[target], q_recv.at[slot], q_sems.at[0], q_sems.at[1], target).start()
        return carry

    lax.fori_loop(1, n_dev, send_query, 0)

    loads[2].wait()

    def send_weight(i, carry):
        other = (chip + i) % n_chip
        remote(wo_v.at[:, pl.ds(pl.multiple_of(other * cols, cols), cols)], wo_c.at[chip, core], wo_sems.at[0], wo_sems.at[1], 2 * other + core).start()
        return carry

    lax.fori_loop(1, n_chip, send_weight, 0)
    wo_c[chip, core] = wo_v[:, pl.ds(pl.multiple_of(chip * cols, cols), cols)]

    loads[3].wait()
    loads[4].wait()

    def project_new(i, accs):
        at = pl.ds(pl.multiple_of(i * k_step, k_step), k_step)
        rows = x_v[:, at]
        return accs[0] + dot_nt(wk_v[:, at], rows), accs[1] + dot_nt(wv_v[:, at], rows)

    zero_new = jnp.zeros((head_dim, n_rows), F32)
    key_all, value_all = lax.fori_loop(0, model_dim // k_step, project_new, (zero_new, zero_new))
    lanes = lax.broadcasted_iota(jnp.int32, (head_dim, n_rows), 1)
    key_new = jnp.sum(jnp.where(lanes == me, key_all, 0.0), axis=1, keepdims=True)
    value_new = jnp.sum(jnp.where(lanes == me, value_all, 0.0), axis=1, keepdims=True)
    key_new = jnp.broadcast_to(key_new, (head_dim, 128)).astype(BF16)
    value_new = jnp.broadcast_to(value_new, (head_dim, 128)).astype(BF16)
    new_ref[0] = key_new
    new_ref[1] = value_new

    loads[5].wait()
    loads[6].wait()
    pltpu.make_async_copy(q_recv.at[pl.ds(0, n_dev - 1)], q_recv.at[pl.ds(0, n_dev - 1)], q_sems.at[0]).wait()
    pltpu.make_async_copy(q_recv.at[pl.ds(0, n_dev - 1)], q_recv.at[pl.ds(0, n_dev - 1)], q_sems.at[1]).wait()

    q_row = q_recv[:, 0, :][:, :head_dim].astype(BF16)
    row_len = len_ref[me]
    scale = (head_dim ** -0.5) * LOG2E
    ident = (lax.broadcasted_iota(jnp.int32, (head_dim, head_dim), 0) == lax.broadcasted_iota(jnp.int32, (head_dim, head_dim), 1)).astype(BF16)
    value_row = dot_nt(jnp.ones((8, head_dim), BF16), ident * value_new[:, :head_dim])[:1]
    s_new = jnp.dot(q_row, key_new, preferred_element_type=F32)[:, :1]
    block = 2048

    def attend(i, state):
        run_max, run_sum, acc = state
        start = pl.multiple_of(i * block, block)
        scores = jnp.dot(q_row, key_v[:, pl.ds(start, block)], preferred_element_type=F32)
        positions = start + lax.broadcasted_iota(jnp.int32, (1, block), 1)
        scores = jnp.where(positions < row_len, scores, -jnp.inf)
        new_max = jnp.maximum(run_max, jnp.max(scores, axis=1, keepdims=True))
        weights = jnp.exp2((scores - new_max) * scale)
        shrink = jnp.exp2((run_max - new_max) * scale)
        run_sum = shrink * run_sum + jnp.sum(weights, axis=1, keepdims=True)
        acc = shrink * acc + dot_nt(weights.astype(BF16), value_v[:, pl.ds(start, block)])
        return new_max, run_sum, acc

    n_heads = q_row.shape[0]
    state = (s_new, jnp.ones((n_heads, 1), F32), jnp.broadcast_to(value_row, (n_heads, head_dim)))
    run_max, run_sum, acc = lax.fori_loop(0, seq_len // block, attend, state)
    ctx = acc / run_sum
    ctx_send[...] = jnp.concatenate([ctx[:n_chip], ctx[n_chip:]], axis=1).astype(BF16)

    row = me % n_chip

    def send_ctx(i, carry):
        target = 2 * ((chip + i) % n_chip) + half
        remote(ctx_send, ctx_recv.at[row], ctx_sems.at[0], ctx_in.at[row], target).start()
        return carry

    lax.fori_loop(1, n_chip, send_ctx, 0)

    @pl.when(core != half)
    def _():
        remote(ctx_send, ctx_recv.at[row], ctx_sems.at[1], ctx_in.at[row], 2 * chip + half).start()

    @pl.when(core == half)
    def _():
        ctx_recv[row] = ctx_send[...]

    weight_half = wo_c.at[pl.ds(0, n_chip - 1), 0]
    pltpu.make_async_copy(weight_half, weight_half, wo_sems.at[0]).wait()
    pltpu.make_async_copy(weight_half, weight_half, wo_sems.at[1]).wait()
    partner = 2 * chip + 1 - core
    swap = remote(wo_c.at[:, core], wo_c.at[:, core], wo_sems.at[2], wo_sems.at[3], partner)
    swap.start()

    def widen(r):
        ctx_wide[pl.ds(pl.multiple_of(r * n_chip, n_chip), n_chip)] = ctx_recv[r].astype(F32)

    def take_ctx(i, carry):
        r = (me + n_dev - i) % n_chip

        @pl.when((core != half) | (i != 0))
        def _():
            pltpu.make_async_copy(ctx_recv.at[r], ctx_recv.at[r], ctx_in.at[r]).wait()

        widen(r)
        return carry

    lax.fori_loop(0, n_chip, take_ctx, 0)
    for h in range(n_chip):
        ctx_all[:, h * cols:(h + 1) * cols] = ctx_wide[pl.ds(h, half_rows, stride=n_chip), :].astype(BF16)

    swap.wait()
    k_chips = 8

    def out_step(i, total):
        lhs = ctx_all[:, pl.ds(pl.multiple_of(i * k_chips * cols, k_chips * cols), k_chips * cols)]
        rhs = wo_c[pl.ds(i * k_chips, k_chips)].reshape(k_chips * cols, cols)
        return total + jnp.dot(lhs, rhs, preferred_element_type=F32)

    total = lax.fori_loop(0, n_chip // k_chips, out_step, jnp.zeros((half_rows, cols), F32))
    my_rows = pl.ds(pl.multiple_of(core * half_rows, half_rows), half_rows)
    other_rows = pl.ds(pl.multiple_of((1 - core) * half_rows, half_rows), half_rows)

    def col_block(c):
        return pl.ds(pl.multiple_of(c * cols, cols), cols)

    total = total + x_v[my_rows, col_block(chip)].astype(F32)
    out_send[...] = total.astype(BF16)

    def send_out(i, carry):
        other = (chip + i) % n_chip
        remote(out_send, out_ref.at[my_rows, col_block(chip)], out_sems.at[0], out_in.at[chip], 2 * other + core).start()
        return carry

    lax.fori_loop(1, n_chip, send_out, 0)
    out_ref[my_rows, col_block(chip)] = out_send[...]
    remote(out_send, out_ref.at[my_rows, col_block(chip)], out_sems.at[1], out_sems.at[2], partner).start()

    def pass_on(i, carry):
        c = (chip + n_chip - i) % n_chip
        piece = out_ref.at[my_rows, col_block(c)]
        pltpu.make_async_copy(piece, piece, out_in.at[c]).wait()
        remote(piece, piece, out_sems.at[1], out_sems.at[2], partner).start()
        return carry

    lax.fori_loop(1, n_chip, pass_on, 0)

    ctx_part = ctx_recv.at[pl.ds(0, n_chip - 1)]
    pltpu.make_async_copy(ctx_part, ctx_part, ctx_sems.at[0]).wait()

    @pl.when(core != half)
    def _():
        pltpu.make_async_copy(ctx_send, ctx_send, ctx_sems.at[1]).wait()

    pltpu.make_async_copy(ctx_part, ctx_part, out_sems.at[0]).wait()
    pltpu.make_async_copy(out_ref.at[my_rows], out_ref.at[my_rows], out_sems.at[1]).wait()
    pltpu.make_async_copy(out_ref.at[other_rows], out_ref.at[other_rows], out_sems.at[2]).wait()


def step(x, wq_t, wk_t, wv_t, wo, key_t, value_t, lengths, n_dev):
    n_rows, model_dim = x.shape
    head_dim, seq_len = key_t.shape
    n_chip = n_dev // 2
    cols = model_dim // n_chip
    dma = pltpu.SemaphoreType.DMA
    return pl.pallas_call(
        functools.partial(step_kernel, n_dev),
        out_shape=(jax.ShapeDtypeStruct(x.shape, BF16), jax.ShapeDtypeStruct((2, head_dim, 128), BF16)),
        in_specs=[pl.BlockSpec(memory_space=pl.ANY)] * 7 + [pl.BlockSpec(memory_space=pltpu.SMEM)],
        out_specs=(pl.BlockSpec(memory_space=pltpu.VMEM), pl.BlockSpec(memory_space=pltpu.VMEM)),
        scratch_shapes=[
            pltpu.VMEM(x.shape, BF16), pltpu.VMEM(wq_t.shape, BF16), pltpu.VMEM(wk_t.shape, BF16), pltpu.VMEM(wv_t.shape, BF16),
            pltpu.VMEM(wo.shape, BF16), pltpu.VMEM(key_t.shape, BF16), pltpu.VMEM(value_t.shape, BF16),
            pltpu.VMEM((n_dev, 1, 128), F32), pltpu.VMEM((n_dev, 1, 128), F32),
            pltpu.VMEM((n_chip, 2, head_dim, cols), BF16),
            pltpu.VMEM((n_chip, cols), BF16), pltpu.VMEM((n_chip, n_chip, cols), BF16), pltpu.VMEM((n_chip * n_chip, cols), F32),
            pltpu.VMEM((n_rows // 2, model_dim), BF16), pltpu.VMEM((n_rows // 2, cols), BF16),
            dma((7,)), dma((2,)), dma((4,)), dma((2,)), dma((n_chip,)), dma((3,)), dma((n_chip,)),
        ],
        compiler_params=pltpu.CompilerParams(collective_id=0, has_side_effects=True, vmem_limit_bytes=48 * 1024 * 1024),
        name='decode_step',
    )(x, wq_t, wk_t, wv_t, wo, key_t, value_t, lengths)


def cache_kernel(len_ref, new_ref, key_hbm, value_hbm, key_out, value_out, buf, in_sem, out_sem):
    row = lax.axis_index('model')
    head_dim, seq_len = key_hbm.shape
    n_piece = 4
    width = seq_len // n_piece
    ins, outs = [], []
    for n in range(2 * n_piece):
        src, dst = ((key_hbm, key_out), (value_hbm, value_out))[n % 2]
        at = pl.ds((n // 2) * width, width)
        ins.append(pltpu.make_async_copy(src.at[:, at], buf.at[n], in_sem.at[n]))
        outs.append(pltpu.make_async_copy(buf.at[n], dst.at[:, at], out_sem.at[n]))
        ins[n].start()
    pos = len_ref[row]
    lanes = lax.broadcasted_iota(jnp.int32, (head_dim, 128), 1)
    for n in range(2 * n_piece):
        ins[n].wait()
        local = pos - (n // 2) * width

        @pl.when((local >= 0) & (local < width))
        def _():
            at = pl.ds(pl.multiple_of((local // 128) * 128, 128), 128)
            old = buf[n, :, at].astype(F32)
            buf[n, :, at] = jnp.where(lanes == local % 128, new_ref[n % 2].astype(F32), old).astype(BF16)

        outs[n].start()
    for n in range(2 * n_piece):
        outs[n].wait()


def write_cache(lengths, new, key_t, value_t):
    hbm = pl.BlockSpec(memory_space=pl.ANY)
    head_dim, seq_len = key_t.shape
    shape = jax.ShapeDtypeStruct(key_t.shape, BF16)
    return pl.pallas_call(
        cache_kernel,
        out_shape=(shape, shape),
        in_specs=[pl.BlockSpec(memory_space=pltpu.SMEM), pl.BlockSpec(memory_space=pltpu.VMEM), hbm, hbm],
        out_specs=(hbm, hbm),
        scratch_shapes=[pltpu.VMEM((8, head_dim, seq_len // 4), BF16), pltpu.SemaphoreType.DMA((8,)), pltpu.SemaphoreType.DMA((8,))],
        name='cache_write',
    )(lengths, new, key_t, value_t)


def solution(mesh):
    n_dev = mesh.shape['model']

    def group_step(hidden, w_query, w_key, w_value, w_out, key_cache, value_cache, lengths):
        key_t = key_cache[0].T
        value_t = value_cache[0].T
        out, new = step(hidden, w_query.T, w_key.T, w_value.T, w_out, key_t, value_t, lengths, n_dev)
        key_new, value_new = write_cache(lengths, new, key_t, value_t)
        return out, key_new.T[None], value_new.T[None]

    row_spec = P('replica', None)
    cache_spec = P(('replica', 'model'), None, None)
    return jax.shard_map(group_step, mesh=mesh, in_specs=(row_spec, P(None, 'model'), P(None, None), P(None, None), P('model', None), cache_spec, cache_spec, P('replica')), out_specs=(row_spec, cache_spec, cache_spec), check_vma=False)
```

```python
import functools
import jax
import jax.numpy as jnp
from jax import lax
from jax.experimental import pallas as pl
from jax.experimental.pallas import tpu as pltpu
from jax.sharding import PartitionSpec as P

F32 = jnp.float32
BF16 = jnp.bfloat16
NT = (((1,), (1,)), ((), ()))
LOG2E = 1.4426950408889634
VMEM_MIB = 56
FINISH_MIB = 16


def dot_nt(lhs, rhs):
    return lax.dot_general(lhs, rhs, NT, preferred_element_type=F32)


def step_kernel(n_dev, x_hbm, wq_hbm, wk_hbm, wv_hbm, wo_hbm, key_hbm, value_hbm, len_ref, out_ref, new_ref, key_v, value_v,
                x_v, wq_v, wk_v, wv_v, wo_v, q_send, q_recv, wo_send, wo_c, ctx_send, ctx_recv, ctx_wide, ctx_all, out_send, out_recv, scores,
                load_sem, q_sems, wo_sems, ctx_sems, ctx_in, out_sems, out_in):
    me = lax.axis_index('model')
    core = me % 2
    chip = me // 2
    n_chip = n_dev // 2
    half = me // n_chip
    n_rows, model_dim = x_v.shape
    head_dim, seq_len = key_v.shape
    cols = model_dim // n_chip
    half_rows = n_rows // 2

    def remote(src, dst, send_sem, recv_sem, target):
        return pltpu.make_async_remote_copy(src_ref=src, dst_ref=dst, send_sem=send_sem, recv_sem=recv_sem, device_id={'model': target})

    loads = []
    for n, (src, dst) in enumerate(((x_hbm, x_v), (wq_hbm, wq_v), (wo_hbm, wo_v), (wk_hbm, wk_v), (wv_hbm, wv_v), (key_hbm, key_v), (value_hbm, value_v))):
        copy = pltpu.make_async_copy(src, dst, load_sem.at[n])
        loads.append(copy)
    for copy in loads[:3]:
        copy.start()

    barrier = pltpu.get_barrier_semaphore()

    def far_first(i):
        return 1 + (i + 80) % (n_dev - 1)

    def greet(i, carry):
        pl.semaphore_signal(barrier, inc=1, device_id={'model': (me + far_first(i)) % n_dev})
        return carry

    lax.fori_loop(0, n_dev - 1, greet, 0, unroll=True)

    for copy in loads[3:]:
        copy.start()

    loads[0].wait()
    loads[1].wait()
    k_step = 1024

    def project(i, acc):
        at = pl.ds(pl.multiple_of(i * k_step, k_step), k_step)
        return acc + dot_nt(x_v[:, at], wq_v[:, at])

    query = lax.fori_loop(0, model_dim // k_step, project, jnp.zeros((n_rows, head_dim), F32))
    query = query.astype(BF16).astype(F32)
    q_send[:, 0, :] = jnp.concatenate([query, jnp.zeros_like(query)], axis=1)
    slot = core * n_chip + chip
    q_recv[slot] = q_send[me]
    loads[2].wait()
    for c in range(n_chip):
        wo_send[c] = wo_v[:, c * cols:(c + 1) * cols]
    pl.semaphore_wait(barrier, n_dev - 1)

    def send_query(i, carry):
        target = (me + far_first(i)) % n_dev
        remote(q_send.at[target], q_recv.at[slot], q_sems.at[0], q_sems.at[1], target).start()
        return carry

    lax.fori_loop(0, n_dev - 1, send_query, 0, unroll=4)


    def send_weight(i, carry):
        other = (chip + i) % n_chip
        remote(wo_send.at[other], wo_c.at[chip, core], wo_sems.at[0], wo_sems.at[1], 2 * other + core).start()
        return carry

    lax.fori_loop(1, n_chip, send_weight, 0)
    wo_c[chip, core] = wo_send[chip]

    loads[3].wait()
    loads[4].wait()

    def project_new(i, accs):
        at = pl.ds(pl.multiple_of(i * k_step, k_step), k_step)
        rows = x_v[:, at]
        return accs[0] + dot_nt(wk_v[:, at], rows), accs[1] + dot_nt(wv_v[:, at], rows)

    zero_new = jnp.zeros((head_dim, n_rows), F32)
    key_all, value_all = lax.fori_loop(0, model_dim // k_step, project_new, (zero_new, zero_new))
    lanes = lax.broadcasted_iota(jnp.int32, (head_dim, n_rows), 1)
    key_new = jnp.sum(jnp.where(lanes == me, key_all, 0.0), axis=1, keepdims=True)
    value_new = jnp.sum(jnp.where(lanes == me, value_all, 0.0), axis=1, keepdims=True)
    key_new = jnp.broadcast_to(key_new, (head_dim, 128)).astype(BF16)
    value_new = jnp.broadcast_to(value_new, (head_dim, 128)).astype(BF16)
    new_ref[0] = key_new
    new_ref[1] = value_new

    loads[5].wait()
    loads[6].wait()
    pltpu.make_async_copy(q_recv.at[pl.ds(0, n_dev - 1)], q_recv.at[pl.ds(0, n_dev - 1)], q_sems.at[0]).wait()
    pltpu.make_async_copy(q_recv.at[pl.ds(0, n_dev - 1)], q_recv.at[pl.ds(0, n_dev - 1)], q_sems.at[1]).wait()

    q_row = q_recv[:, 0, :][:, :head_dim].astype(BF16)
    row_len = len_ref[me]
    scale = (head_dim ** -0.5) * LOG2E
    ident = (lax.broadcasted_iota(jnp.int32, (head_dim, head_dim), 0) == lax.broadcasted_iota(jnp.int32, (head_dim, head_dim), 1)).astype(BF16)
    value_row = dot_nt(jnp.ones((8, head_dim), BF16), ident * value_new[:, :head_dim])[:1]
    s_new = jnp.dot(q_row, key_new, preferred_element_type=F32)[:, :1]
    block = 2048
    n_heads = q_row.shape[0]
    lane_pos = lax.broadcasted_iota(jnp.int32, (1, block), 1)

    def fold(op, array):
        parts = [array[:, n * 128:(n + 1) * 128] for n in range(array.shape[1] // 128)]
        while len(parts) > 1:
            parts = [op(parts[n], parts[n + 1]) for n in range(0, len(parts), 2)]
        return parts[0]

    def score(i, lane_max):
        start = pl.multiple_of(i * block, block)
        part = jnp.dot(q_row, key_v[:, pl.ds(start, block)], preferred_element_type=F32)
        part = jnp.where(lane_pos + start < row_len, part, -jnp.inf)
        scores[:, pl.ds(start, block)] = part
        return jnp.maximum(lane_max, fold(jnp.maximum, part))

    lane_max = lax.fori_loop(0, seq_len // block, score, jnp.broadcast_to(s_new, (n_heads, 128)))
    row_max = jnp.max(lane_max, axis=1, keepdims=True)

    def weigh(i, state):
        lane_sum, acc = state
        start = pl.multiple_of(i * block, block)
        weights = jnp.exp2((scores[:, pl.ds(start, block)] - row_max) * scale)
        acc = acc + dot_nt(weights.astype(BF16), value_v[:, pl.ds(start, block)])
        return lane_sum + fold(jnp.add, weights), acc

    first = jnp.exp2((s_new - row_max) * scale)
    state = (jnp.zeros((n_heads, 128), F32), first.astype(BF16).astype(F32) * value_row)
    lane_sum, acc = lax.fori_loop(0, seq_len // block, weigh, state)
    run_sum = first + jnp.sum(lane_sum, axis=1, keepdims=True)
    ctx = acc / run_sum
    ctx_send[...] = jnp.concatenate([ctx[:n_chip], ctx[n_chip:]], axis=1).astype(BF16)

    row = me % n_chip

    def send_ctx(i, carry):
        target = 2 * ((chip + i) % n_chip) + half
        remote(ctx_send, ctx_recv.at[row], ctx_sems.at[0], ctx_in.at[row], target).start()
        return carry

    lax.fori_loop(1, n_chip, send_ctx, 0)

    @pl.when(core != half)
    def _():
        remote(ctx_send, ctx_recv.at[row], ctx_sems.at[1], ctx_in.at[row], 2 * chip + half).start()

    @pl.when(core == half)
    def _():
        ctx_recv[row] = ctx_send[...]

    weight_half = wo_c.at[pl.ds(0, n_chip - 1), 0]
    pltpu.make_async_copy(weight_half, weight_half, wo_sems.at[0]).wait()
    pltpu.make_async_copy(weight_half, weight_half, wo_sems.at[1]).wait()
    partner = 2 * chip + 1 - core
    swap = remote(wo_c.at[:, core], wo_c.at[:, core], wo_sems.at[2], wo_sems.at[3], partner)
    swap.start()

    def widen(r):
        ctx_wide[pl.ds(pl.multiple_of(r * n_chip, n_chip), n_chip)] = ctx_recv[r].astype(F32)

    def take_ctx(i, carry):
        r = (me + n_dev - i) % n_chip

        @pl.when((core != half) | (i != 0))
        def _():
            pltpu.make_async_copy(ctx_recv.at[r], ctx_recv.at[r], ctx_in.at[r]).wait()

        widen(r)
        return carry

    lax.fori_loop(0, n_chip, take_ctx, 0)
    for h in range(n_chip):
        ctx_all[:, h * cols:(h + 1) * cols] = ctx_wide[pl.ds(h, half_rows, stride=n_chip), :].astype(BF16)

    swap.wait()
    k_chips = 8

    def out_step(i, total):
        lhs = ctx_all[:, pl.ds(pl.multiple_of(i * k_chips * cols, k_chips * cols), k_chips * cols)]
        rhs = wo_c[pl.ds(i * k_chips, k_chips)].reshape(k_chips * cols, cols)
        return total + jnp.dot(lhs, rhs, preferred_element_type=F32)

    total = lax.fori_loop(0, n_chip // k_chips, out_step, jnp.zeros((half_rows, cols), F32))
    my_rows = pl.ds(pl.multiple_of(core * half_rows, half_rows), half_rows)
    other_rows = pl.ds(pl.multiple_of((1 - core) * half_rows, half_rows), half_rows)

    def col_block(c):
        return pl.ds(pl.multiple_of(c * cols, cols), cols)

    total = total + x_v[my_rows, col_block(chip)].astype(F32)
    out_send[...] = total.astype(BF16)

    def send_out(i, carry):
        other = (chip + i) % n_chip
        remote(out_send, out_recv.at[core, chip], out_sems.at[0], out_in.at[chip], 2 * other + core).start()
        return carry

    lax.fori_loop(1, n_chip, send_out, 0)
    remote(out_send, out_recv.at[core, chip], out_sems.at[1], out_sems.at[2], partner).start()
    out_ref[my_rows, col_block(chip)] = out_send[...]

    def pass_on(i, carry):
        c = (chip + n_chip - i) % n_chip
        piece = out_recv.at[core, c]
        pltpu.make_async_copy(piece, piece, out_in.at[c]).wait()
        remote(piece, piece, out_sems.at[1], out_sems.at[2], partner).start()
        out_ref[my_rows, col_block(c)] = out_recv[core, c]
        return carry

    lax.fori_loop(1, n_chip, pass_on, 0)

    ctx_part = ctx_recv.at[pl.ds(0, n_chip - 1)]
    pltpu.make_async_copy(ctx_part, ctx_part, ctx_sems.at[0]).wait()

    @pl.when(core != half)
    def _():
        pltpu.make_async_copy(ctx_send, ctx_send, ctx_sems.at[1]).wait()

    pltpu.make_async_copy(ctx_part, ctx_part, out_sems.at[0]).wait()
    pltpu.make_async_copy(out_recv.at[0], out_recv.at[0], out_sems.at[1]).wait()
    pltpu.make_async_copy(out_recv.at[1], out_recv.at[1], out_sems.at[2]).wait()
    for c in range(n_chip):
        out_ref[other_rows, c * cols:(c + 1) * cols] = out_recv[1 - core, c]


def step(x, wq_t, wk_t, wv_t, wo, key_t, value_t, lengths, n_dev):
    n_rows, model_dim = x.shape
    head_dim, seq_len = key_t.shape
    n_chip = n_dev // 2
    cols = model_dim // n_chip
    dma = pltpu.SemaphoreType.DMA
    return pl.pallas_call(
        functools.partial(step_kernel, n_dev),
        out_shape=(pltpu.VMEM(x.shape, BF16), pltpu.VMEM((2, head_dim, 128), BF16), pltpu.VMEM(key_t.shape, BF16), pltpu.VMEM(value_t.shape, BF16)),
        in_specs=[pl.BlockSpec(memory_space=pltpu.HBM)] * 7 + [pl.BlockSpec(memory_space=pltpu.SMEM)],
        out_specs=(pl.BlockSpec(memory_space=pltpu.VMEM),) * 4,
        scratch_shapes=[
            pltpu.VMEM(x.shape, BF16), pltpu.VMEM(wq_t.shape, BF16), pltpu.VMEM(wk_t.shape, BF16), pltpu.VMEM(wv_t.shape, BF16),
            pltpu.VMEM(wo.shape, BF16),
            pltpu.VMEM((n_dev, 1, 128), F32), pltpu.VMEM((n_dev, 1, 128), F32),
            pltpu.VMEM((n_chip, head_dim, cols), BF16),
            pltpu.VMEM((n_chip, 2, head_dim, cols), BF16),
            pltpu.VMEM((n_chip, cols), BF16), pltpu.VMEM((n_chip, n_chip, cols), BF16), pltpu.VMEM((n_chip * n_chip, cols), F32),
            pltpu.VMEM((n_rows // 2, model_dim), BF16), pltpu.VMEM((n_rows // 2, cols), BF16),
            pltpu.VMEM((2, n_chip, n_rows // 2, cols), BF16), pltpu.VMEM((n_dev, seq_len), F32),
            dma((7,)), dma((2,)), dma((4,)), dma((2,)), dma((n_chip,)), dma((3,)), dma((n_chip,)),
        ],
        compiler_params=pltpu.CompilerParams(collective_id=0, has_side_effects=True, vmem_limit_bytes=VMEM_MIB * 1024 * 1024),
        name='decode_step',
    )(x, wq_t, wk_t, wv_t, wo, key_t, value_t, lengths)


def finish_kernel(len_ref, out_v, new_ref, key_v, value_v, out_hbm, key_hbm, value_hbm, key_tile, value_tile, sems):
    row = lax.axis_index('model')
    head_dim, seq_len = key_v.shape
    pairs = ((out_v, out_hbm), (key_v, key_hbm), (value_v, value_hbm))
    copies = [pltpu.make_async_copy(src, dst, sems.at[n]) for n, (src, dst) in enumerate(pairs)]
    for copy in copies:
        copy.start()
    pos = len_ref[row]
    at = pl.ds(pl.multiple_of((pos // 128) * 128, 128), 128)
    hit = lax.broadcasted_iota(jnp.int32, (head_dim, 128), 1) == pos % 128
    key_tile[...] = jnp.where(hit, new_ref[0].astype(F32), key_v[:, at].astype(F32)).astype(BF16)
    value_tile[...] = jnp.where(hit, new_ref[1].astype(F32), value_v[:, at].astype(F32)).astype(BF16)
    for copy in copies[1:]:
        copy.wait()
    tiles = [pltpu.make_async_copy(key_tile, key_hbm.at[:, at], sems.at[3]), pltpu.make_async_copy(value_tile, value_hbm.at[:, at], sems.at[4])]
    for copy in tiles:
        copy.start()
    copies[0].wait()
    for copy in tiles:
        copy.wait()


def finish(lengths, out, new, key_v, value_v):
    hbm = pl.BlockSpec(memory_space=pltpu.HBM)
    vmem = pl.BlockSpec(memory_space=pltpu.VMEM)
    head_dim = key_v.shape[0]
    return pl.pallas_call(
        finish_kernel,
        out_shape=tuple(jax.ShapeDtypeStruct(a.shape, BF16) for a in (out, key_v, value_v)),
        in_specs=[pl.BlockSpec(memory_space=pltpu.SMEM), vmem, vmem, vmem, vmem],
        out_specs=(hbm, hbm, hbm),
        scratch_shapes=[pltpu.VMEM((head_dim, 128), BF16), pltpu.VMEM((head_dim, 128), BF16), pltpu.SemaphoreType.DMA((5,))],
        compiler_params=pltpu.CompilerParams(vmem_limit_bytes=FINISH_MIB * 1024 * 1024),
        name='finish',
    )(lengths, out, new, key_v, value_v)


def solution(mesh):
    n_dev = mesh.shape['model']

    def group_step(hidden, w_query, w_key, w_value, w_out, key_cache, value_cache, lengths):
        key_t = key_cache[0].T
        value_t = value_cache[0].T
        out, new, key_v, value_v = step(hidden, w_query.T, w_key.T, w_value.T, w_out, key_t, value_t, lengths, n_dev)
        out, key_new, value_new = finish(lengths, out, new, key_v, value_v)
        return out, key_new.T[None], value_new.T[None]

    row_spec = P('replica', None)
    cache_spec = P(('replica', 'model'), None, None)
    return jax.shard_map(group_step, mesh=mesh, in_specs=(row_spec, P(None, 'model'), P(None, None), P(None, None), P('model', None), cache_spec, cache_spec, P('replica')), out_specs=(row_spec, cache_spec, cache_spec), check_vma=False)
```

```python
import functools
import jax
import jax.numpy as jnp
from jax import lax
from jax.experimental import pallas as pl
from jax.experimental.pallas import tpu as pltpu
from jax.sharding import PartitionSpec as P

F32 = jnp.float32
BF16 = jnp.bfloat16
NT = (((1,), (1,)), ((), ()))
LOG2E = 1.4426950408889634
VMEM_MIB = 56
N_GRP = 4
FINISH_MIB = 16


def dot_nt(lhs, rhs):
    return lax.dot_general(lhs, rhs, NT, preferred_element_type=F32)


def step_kernel(n_dev, n_grp, x_hbm, wq_hbm, wk_hbm, wv_hbm, wo_hbm, key_hbm, value_hbm, len_ref, out_ref, key_v, value_v,
                x_v, wq_v, wk_v, wv_v, wo_v, q_send, q_recv, wo_send, wo_c, ctx_send, ctx_recv, ctx_wide, ctx_all, part_own, part_send, part_recv, out_send, out_recv, scores,
                load_sem, q_sems, wo_sems, ctx_sems, ctx_in, part_sems, out_sems, out_in):
    me = lax.axis_index('model')
    core = me % 2
    chip = me // 2
    n_chip = n_dev // 2
    half = me // n_chip
    n_rows, model_dim = x_v.shape
    head_dim, seq_len = key_v.shape
    cols = model_dim // n_chip
    half_rows = n_rows // 2
    plane = n_chip // n_grp
    group = chip // plane
    spot = chip % plane
    wide_cols = cols * n_grp

    def remote(src, dst, send_sem, recv_sem, target):
        return pltpu.make_async_remote_copy(src_ref=src, dst_ref=dst, send_sem=send_sem, recv_sem=recv_sem, device_id={'model': target})

    loads = []
    for n, (src, dst) in enumerate(((x_hbm, x_v), (wq_hbm, wq_v), (wo_hbm, wo_v), (wk_hbm, wk_v), (wv_hbm, wv_v), (key_hbm, key_v), (value_hbm, value_v))):
        copy = pltpu.make_async_copy(src, dst, load_sem.at[n])
        loads.append(copy)
    for copy in loads[:3]:
        copy.start()

    barrier = pltpu.get_barrier_semaphore()

    def far_first(i):
        return 1 + (i + 80) % (n_dev - 1)

    def greet(i, carry):
        pl.semaphore_signal(barrier, inc=1, device_id={'model': (me + far_first(i)) % n_dev})
        return carry

    lax.fori_loop(0, n_dev - 1, greet, 0, unroll=True)

    for copy in loads[3:]:
        copy.start()

    loads[0].wait()
    loads[1].wait()
    k_step = 1024

    def project(i, acc):
        at = pl.ds(pl.multiple_of(i * k_step, k_step), k_step)
        return acc + dot_nt(x_v[:, at], wq_v[:, at])

    query = lax.fori_loop(0, model_dim // k_step, project, jnp.zeros((n_rows, head_dim), F32))
    query = query.astype(BF16).astype(F32)
    q_send[:, 0, :] = jnp.concatenate([query, jnp.zeros_like(query)], axis=1)
    slot = core * n_chip + chip
    q_recv[slot] = q_send[me]
    loads[2].wait()
    for c in range(plane):
        wo_send[c] = wo_v[:, c * wide_cols:(c + 1) * wide_cols]
    pl.semaphore_wait(barrier, n_dev - 1)

    def send_query(i, carry):
        target = (me + far_first(i)) % n_dev
        remote(q_send.at[target], q_recv.at[slot], q_sems.at[0], q_sems.at[1], target).start()
        return carry

    lax.fori_loop(0, n_dev - 1, send_query, 0, unroll=4)

    def send_weight(i, carry):
        other = (spot + i) % plane
        remote(wo_send.at[other], wo_c.at[spot, core], wo_sems.at[0], wo_sems.at[1], 2 * (group * plane + other) + core).start()
        return carry

    lax.fori_loop(1, plane, send_weight, 0)
    wo_c[spot, core] = wo_send[spot]

    loads[3].wait()
    loads[4].wait()

    def project_new(i, accs):
        at = pl.ds(pl.multiple_of(i * k_step, k_step), k_step)
        rows = x_v[:, at]
        return accs[0] + dot_nt(wk_v[:, at], rows), accs[1] + dot_nt(wv_v[:, at], rows)

    zero_new = jnp.zeros((head_dim, n_rows), F32)
    key_all, value_all = lax.fori_loop(0, model_dim // k_step, project_new, (zero_new, zero_new))
    lanes = lax.broadcasted_iota(jnp.int32, (head_dim, n_rows), 1)
    key_new = jnp.sum(jnp.where(lanes == me, key_all, 0.0), axis=1, keepdims=True)
    value_new = jnp.sum(jnp.where(lanes == me, value_all, 0.0), axis=1, keepdims=True)
    key_new = jnp.broadcast_to(key_new, (head_dim, 128)).astype(BF16)
    value_new = jnp.broadcast_to(value_new, (head_dim, 128)).astype(BF16)

    loads[5].wait()
    loads[6].wait()
    pltpu.make_async_copy(q_recv.at[pl.ds(0, n_dev - 1)], q_recv.at[pl.ds(0, n_dev - 1)], q_sems.at[0]).wait()
    pltpu.make_async_copy(q_recv.at[pl.ds(0, n_dev - 1)], q_recv.at[pl.ds(0, n_dev - 1)], q_sems.at[1]).wait()

    q_row = q_recv[:, 0, :][:, :head_dim].astype(BF16)
    row_len = len_ref[me]
    scale = (head_dim ** -0.5) * LOG2E
    ident = (lax.broadcasted_iota(jnp.int32, (head_dim, head_dim), 0) == lax.broadcasted_iota(jnp.int32, (head_dim, head_dim), 1)).astype(BF16)
    value_row = dot_nt(jnp.ones((8, head_dim), BF16), ident * value_new[:, :head_dim])[:1]
    s_new = jnp.dot(q_row, key_new, preferred_element_type=F32)[:, :1]
    block = 2048
    n_heads = q_row.shape[0]
    lane_pos = lax.broadcasted_iota(jnp.int32, (1, block), 1)

    def fold(op, array):
        parts = [array[:, n * 128:(n + 1) * 128] for n in range(array.shape[1] // 128)]
        while len(parts) > 1:
            parts = [op(parts[n], parts[n + 1]) for n in range(0, len(parts), 2)]
        return parts[0]

    def score(i, lane_max):
        start = pl.multiple_of(i * block, block)
        part = jnp.dot(q_row, key_v[:, pl.ds(start, block)], preferred_element_type=F32)
        part = jnp.where(lane_pos + start < row_len, part, -jnp.inf)
        scores[:, pl.ds(start, block)] = part
        return jnp.maximum(lane_max, fold(jnp.maximum, part))

    lane_max = lax.fori_loop(0, seq_len // block, score, jnp.broadcast_to(s_new, (n_heads, 128)))
    row_max = jnp.max(lane_max, axis=1, keepdims=True)

    def weigh(i, state):
        lane_sum, acc = state
        start = pl.multiple_of(i * block, block)
        weights = jnp.exp2((scores[:, pl.ds(start, block)] - row_max) * scale)
        acc = acc + dot_nt(weights.astype(BF16), value_v[:, pl.ds(start, block)])
        return lane_sum + fold(jnp.add, weights), acc

    first = jnp.exp2((s_new - row_max) * scale)
    state = (jnp.zeros((n_heads, 128), F32), first.astype(BF16).astype(F32) * value_row)
    lane_sum, acc = lax.fori_loop(0, seq_len // block, weigh, state)
    run_sum = first + jnp.sum(lane_sum, axis=1, keepdims=True)
    ctx = acc / run_sum
    ctx_send[...] = jnp.concatenate([ctx[:n_chip], ctx[n_chip:]], axis=1).astype(BF16)

    row = me % n_chip

    def heads_of(c):
        return pl.ds(pl.multiple_of((c // plane) * plane, plane), plane)

    def send_ctx(i, carry):
        other = (chip + i) % n_chip
        remote(ctx_send.at[heads_of(other)], ctx_recv.at[row], ctx_sems.at[0], ctx_in.at[row], 2 * other + half).start()
        return carry

    lax.fori_loop(1, n_chip, send_ctx, 0)

    @pl.when(core != half)
    def _():
        remote(ctx_send.at[heads_of(chip)], ctx_recv.at[row], ctx_sems.at[1], ctx_in.at[row], 2 * chip + half).start()

    @pl.when(core == half)
    def _():
        ctx_recv[row] = ctx_send[heads_of(chip)]

    fix_block = 1024
    fix_pos = lax.broadcasted_iota(jnp.int32, (1, fix_block), 1)
    key_cols = jnp.concatenate([key_new] * (fix_block // 128), axis=1)
    value_cols = jnp.concatenate([value_new] * (fix_block // 128), axis=1)

    def fix(i, carry):
        start = pl.multiple_of(i * fix_block, fix_block)
        at = pl.ds(start, fix_block)
        hit = jnp.broadcast_to(fix_pos + start == row_len, (head_dim, fix_block))
        key_v[:, at] = jnp.where(hit, key_cols, key_v[:, at])
        value_v[:, at] = jnp.where(hit, value_cols, value_v[:, at])
        return carry

    lax.fori_loop(0, seq_len // fix_block, fix, 0)

    weight_half = wo_c.at[pl.ds(0, plane - 1), 0]
    pltpu.make_async_copy(weight_half, weight_half, wo_sems.at[0]).wait()
    pltpu.make_async_copy(weight_half, weight_half, wo_sems.at[1]).wait()
    partner = 2 * chip + 1 - core
    swap = remote(wo_c.at[:, core], wo_c.at[:, core], wo_sems.at[2], wo_sems.at[3], partner)
    swap.start()

    def widen(r):
        ctx_wide[pl.ds(pl.multiple_of(r * plane, plane), plane)] = ctx_recv[r].astype(F32)

    def take_ctx(i, carry):
        r = (me + n_dev - i) % n_chip

        @pl.when((core != half) | (i != 0))
        def _():
            pltpu.make_async_copy(ctx_recv.at[r], ctx_recv.at[r], ctx_in.at[r]).wait()

        widen(r)
        return carry

    lax.fori_loop(0, n_chip, take_ctx, 0)
    for h in range(plane):
        ctx_all[:, h * 128:(h + 1) * 128] = ctx_wide[pl.ds(h, half_rows, stride=plane), :].astype(BF16)

    swap.wait()
    k_chips = 4
    total = jnp.zeros((half_rows, wide_cols), F32)
    for n in range(0, plane, k_chips):
        rhs = wo_c[n:n + k_chips].reshape(k_chips * 128, wide_cols)
        total = total + jnp.dot(ctx_all[:, n * 128:(n + k_chips) * 128], rhs, preferred_element_type=F32)
    for j in range(n_grp):
        part_own[j] = total[:, j * cols:(j + 1) * cols]
        part_send[j] = total[:, j * cols:(j + 1) * cols].astype(BF16)
    for i in range(1, n_grp):
        j = (group + i) % n_grp
        remote(part_send.at[j], part_recv.at[group], part_sems.at[0], part_sems.at[1], 2 * (j * plane + spot) + core).start()
    my_rows = pl.ds(pl.multiple_of(core * half_rows, half_rows), half_rows)
    other_rows = pl.ds(pl.multiple_of((1 - core) * half_rows, half_rows), half_rows)

    def col_block(c):
        return pl.ds(pl.multiple_of(((c % plane) * n_grp + c // plane) * cols, cols), cols)

    own = part_own[group] + x_v[my_rows, col_block(chip)].astype(F32)
    part_all = part_recv.at[pl.ds(0, n_grp - 1)]
    pltpu.make_async_copy(part_all, part_all, part_sems.at[1]).wait()
    for i in range(1, n_grp):
        own = own + part_recv[(group + i) % n_grp].astype(F32)
    out_send[...] = own.astype(BF16)

    def send_out(i, carry):
        other = (chip + i) % n_chip
        remote(out_send, out_recv.at[core, chip], out_sems.at[0], out_in.at[chip], 2 * other + core).start()
        return carry

    lax.fori_loop(1, n_chip, send_out, 0)
    remote(out_send, out_recv.at[core, chip], out_sems.at[1], out_sems.at[2], partner).start()
    out_ref[my_rows, col_block(chip)] = out_send[...]

    def pass_on(i, carry):
        c = (chip + n_chip - i) % n_chip
        piece = out_recv.at[core, c]
        pltpu.make_async_copy(piece, piece, out_in.at[c]).wait()
        remote(piece, piece, out_sems.at[1], out_sems.at[2], partner).start()
        out_ref[my_rows, col_block(c)] = out_recv[core, c]
        return carry

    lax.fori_loop(1, n_chip, pass_on, 0)

    ctx_part = ctx_recv.at[pl.ds(0, n_chip - 1)]
    pltpu.make_async_copy(ctx_part, ctx_part, ctx_sems.at[0]).wait()

    @pl.when(core != half)
    def _():
        pltpu.make_async_copy(ctx_recv.at[0], ctx_recv.at[0], ctx_sems.at[1]).wait()

    pltpu.make_async_copy(part_all, part_all, part_sems.at[0]).wait()
    out_part = out_recv.at[0, pl.ds(0, n_chip - 1)]
    pltpu.make_async_copy(out_part, out_part, out_sems.at[0]).wait()
    pltpu.make_async_copy(out_recv.at[0], out_recv.at[0], out_sems.at[1]).wait()
    pltpu.make_async_copy(out_recv.at[1], out_recv.at[1], out_sems.at[2]).wait()
    for c in range(n_chip):
        block_at = ((c % plane) * n_grp + c // plane) * cols
        out_ref[other_rows, block_at:block_at + cols] = out_recv[1 - core, c]


def step(x, wq_t, wk_t, wv_t, wo, key_t, value_t, lengths, n_dev, n_grp):
    n_rows, model_dim = x.shape
    head_dim, seq_len = key_t.shape
    n_chip = n_dev // 2
    cols = model_dim // n_chip
    plane = n_chip // n_grp
    dma = pltpu.SemaphoreType.DMA
    return pl.pallas_call(
        functools.partial(step_kernel, n_dev, n_grp),
        out_shape=(pltpu.VMEM(x.shape, BF16), pltpu.VMEM(key_t.shape, BF16), pltpu.VMEM(value_t.shape, BF16)),
        in_specs=[pl.BlockSpec(memory_space=pltpu.HBM)] * 7 + [pl.BlockSpec(memory_space=pltpu.SMEM)],
        out_specs=(pl.BlockSpec(memory_space=pltpu.VMEM),) * 3,
        scratch_shapes=[
            pltpu.VMEM(x.shape, BF16), pltpu.VMEM(wq_t.shape, BF16), pltpu.VMEM(wk_t.shape, BF16), pltpu.VMEM(wv_t.shape, BF16),
            pltpu.VMEM(wo.shape, BF16),
            pltpu.VMEM((n_dev, 1, 128), F32), pltpu.VMEM((n_dev, 1, 128), F32),
            pltpu.VMEM((plane, head_dim, cols * n_grp), BF16),
            pltpu.VMEM((plane, 2, head_dim, cols * n_grp), BF16),
            pltpu.VMEM((n_chip, 128), BF16), pltpu.VMEM((n_chip, plane, 128), BF16), pltpu.VMEM((n_chip * plane, 128), F32),
            pltpu.VMEM((n_rows // 2, plane * 128), BF16),
            pltpu.VMEM((n_grp, n_rows // 2, cols), F32), pltpu.VMEM((n_grp, n_rows // 2, cols), BF16), pltpu.VMEM((n_grp, n_rows // 2, cols), BF16),
            pltpu.VMEM((n_rows // 2, cols), BF16),
            pltpu.VMEM((2, n_chip, n_rows // 2, cols), BF16), pltpu.VMEM((n_dev, seq_len), F32),
            dma((7,)), dma((2,)), dma((4,)), dma((2,)), dma((n_chip,)), dma((2,)), dma((3,)), dma((n_chip,)),
        ],
        compiler_params=pltpu.CompilerParams(collective_id=0, has_side_effects=True, vmem_limit_bytes=VMEM_MIB * 1024 * 1024),
        name='decode_step',
    )(x, wq_t, wk_t, wv_t, wo, key_t, value_t, lengths)


def finish_kernel(out_v, key_v, value_v, out_hbm, key_hbm, value_hbm, sems):
    pairs = ((out_v, out_hbm), (key_v, key_hbm), (value_v, value_hbm))
    copies = [pltpu.make_async_copy(src, dst, sems.at[n]) for n, (src, dst) in enumerate(pairs)]
    for copy in copies:
        copy.start()
    for copy in copies:
        copy.wait()


def finish(*arrays):
    return pl.pallas_call(
        finish_kernel,
        out_shape=tuple(jax.ShapeDtypeStruct(a.shape, a.dtype) for a in arrays),
        in_specs=[pl.BlockSpec(memory_space=pltpu.VMEM)] * 3,
        out_specs=(pl.BlockSpec(memory_space=pltpu.HBM),) * 3,
        scratch_shapes=[pltpu.SemaphoreType.DMA((3,))],
        compiler_params=pltpu.CompilerParams(vmem_limit_bytes=FINISH_MIB * 1024 * 1024),
        name='finish',
    )(*arrays)


def solution(mesh):
    n_dev = mesh.shape['model']

    def group_step(hidden, w_query, w_key, w_value, w_out, key_cache, value_cache, lengths):
        key_t = key_cache[0].T
        value_t = value_cache[0].T
        out, key_v, value_v = step(hidden, w_query.T, w_key.T, w_value.T, w_out, key_t, value_t, lengths, n_dev, N_GRP)
        out, key_new, value_new = finish(out, key_v, value_v)
        return out, key_new.T[None], value_new.T[None]

    row_spec = P('replica', None)
    cache_spec = P(('replica', 'model'), None, None)
    return jax.shard_map(group_step, mesh=mesh, in_specs=(row_spec, P(None, 'model'), P(None, None), P(None, None), P('model', None), cache_spec, cache_spec, P('replica')), out_specs=(row_spec, cache_spec, cache_spec), check_vma=False)
```

```python
import functools
import jax
import jax.numpy as jnp
from jax import lax
from jax.experimental import pallas as pl
from jax.experimental.pallas import tpu as pltpu
from jax.sharding import PartitionSpec as P

F32 = jnp.float32
BF16 = jnp.bfloat16
NT = (((1,), (1,)), ((), ()))
LOG2E = 1.4426950408889634
VMEM_MIB = 56
N_GRP = 4
SIDE = 4
PLANE_ORDER = ((0, 1), (1, 0), (0, 3), (3, 0), (1, 1), (3, 3), (1, 3), (3, 1), (0, 2), (2, 0), (1, 2), (2, 1), (3, 2), (2, 3), (2, 2))
FINISH_MIB = 16


def dot_nt(lhs, rhs):
    return lax.dot_general(lhs, rhs, NT, preferred_element_type=F32)


def step_kernel(n_dev, n_grp, x_hbm, wq_hbm, wk_hbm, wv_hbm, wo_hbm, key_hbm, value_hbm, len_ref, out_ref, key_v, value_v,
                x_v, wq_v, wk_v, wv_v, wo_v, q_send, q_recv, wo_send, wo_c, ctx_send, ctx_recv, ctx_wide, ctx_all, part_own, part_send, part_recv, out_send, out_recv, scores,
                load_sem, q_sems, wo_sems, ctx_sems, ctx_in, part_sems, out_sems, plane_in, line_in):
    me = lax.axis_index('model')
    core = me % 2
    chip = me // 2
    n_chip = n_dev // 2
    half = me // n_chip
    n_rows, model_dim = x_v.shape
    head_dim, seq_len = key_v.shape
    cols = model_dim // n_chip
    half_rows = n_rows // 2
    plane = n_chip // n_grp
    group = chip // plane
    spot = chip % plane
    wide_cols = cols * n_grp

    def move(c, stride, by):
        at = (c // stride) % SIDE
        return c + ((at + by) % SIDE - at) * stride

    def remote(src, dst, send_sem, recv_sem, target):
        return pltpu.make_async_remote_copy(src_ref=src, dst_ref=dst, send_sem=send_sem, recv_sem=recv_sem, device_id={'model': target})

    loads = []
    for n, (src, dst) in enumerate(((x_hbm, x_v), (wq_hbm, wq_v), (wo_hbm, wo_v), (wk_hbm, wk_v), (wv_hbm, wv_v), (key_hbm, key_v), (value_hbm, value_v))):
        copy = pltpu.make_async_copy(src, dst, load_sem.at[n])
        loads.append(copy)
    for copy in loads[:3]:
        copy.start()

    barrier = pltpu.get_barrier_semaphore()

    def far_first(i):
        return 1 + (i + 80) % (n_dev - 1)

    def greet(i, carry):
        pl.semaphore_signal(barrier, inc=1, device_id={'model': (me + far_first(i)) % n_dev})
        return carry

    lax.fori_loop(0, n_dev - 1, greet, 0, unroll=True)

    for copy in loads[3:]:
        copy.start()

    loads[0].wait()
    loads[1].wait()
    k_step = 1024

    def project(i, acc):
        at = pl.ds(pl.multiple_of(i * k_step, k_step), k_step)
        return acc + dot_nt(x_v[:, at], wq_v[:, at])

    query = lax.fori_loop(0, model_dim // k_step, project, jnp.zeros((n_rows, head_dim), F32))
    query = query.astype(BF16).astype(F32)
    q_send[:, 0, :] = jnp.concatenate([query, jnp.zeros_like(query)], axis=1)
    slot = core * n_chip + chip
    q_recv[slot] = q_send[me]
    loads[2].wait()
    for c in range(plane):
        wo_send[c] = wo_v[:, c * wide_cols:(c + 1) * wide_cols]
    pl.semaphore_wait(barrier, n_dev - 1)

    def send_query(i, carry):
        target = (me + far_first(i)) % n_dev
        remote(q_send.at[target], q_recv.at[slot], q_sems.at[0], q_sems.at[1], target).start()
        return carry

    lax.fori_loop(0, n_dev - 1, send_query, 0, unroll=4)

    for dy, dx in PLANE_ORDER:
        other = move(move(spot, SIDE, dy), 1, dx)
        remote(wo_send.at[other], wo_c.at[spot, core], wo_sems.at[0], wo_sems.at[1], 2 * (group * plane + other) + core).start()
    wo_c[spot, core] = wo_send[spot]

    loads[3].wait()
    loads[4].wait()

    def project_new(i, accs):
        at = pl.ds(pl.multiple_of(i * k_step, k_step), k_step)
        rows = x_v[:, at]
        return accs[0] + dot_nt(wk_v[:, at], rows), accs[1] + dot_nt(wv_v[:, at], rows)

    zero_new = jnp.zeros((head_dim, n_rows), F32)
    key_all, value_all = lax.fori_loop(0, model_dim // k_step, project_new, (zero_new, zero_new))
    lanes = lax.broadcasted_iota(jnp.int32, (head_dim, n_rows), 1)
    key_new = jnp.sum(jnp.where(lanes == me, key_all, 0.0), axis=1, keepdims=True)
    value_new = jnp.sum(jnp.where(lanes == me, value_all, 0.0), axis=1, keepdims=True)
    key_new = jnp.broadcast_to(key_new, (head_dim, 128)).astype(BF16)
    value_new = jnp.broadcast_to(value_new, (head_dim, 128)).astype(BF16)

    loads[5].wait()
    loads[6].wait()
    pltpu.make_async_copy(q_recv.at[pl.ds(0, n_dev - 1)], q_recv.at[pl.ds(0, n_dev - 1)], q_sems.at[0]).wait()
    pltpu.make_async_copy(q_recv.at[pl.ds(0, n_dev - 1)], q_recv.at[pl.ds(0, n_dev - 1)], q_sems.at[1]).wait()

    q_row = q_recv[:, 0, :][:, :head_dim].astype(BF16)
    row_len = len_ref[me]
    scale = (head_dim ** -0.5) * LOG2E
    ident = (lax.broadcasted_iota(jnp.int32, (head_dim, head_dim), 0) == lax.broadcasted_iota(jnp.int32, (head_dim, head_dim), 1)).astype(BF16)
    value_row = dot_nt(jnp.ones((8, head_dim), BF16), ident * value_new[:, :head_dim])[:1]
    s_new = jnp.dot(q_row, key_new, preferred_element_type=F32)[:, :1]
    block = 2048
    n_heads = q_row.shape[0]
    lane_pos = lax.broadcasted_iota(jnp.int32, (1, block), 1)

    def fold(op, array):
        parts = [array[:, n * 128:(n + 1) * 128] for n in range(array.shape[1] // 128)]
        while len(parts) > 1:
            parts = [op(parts[n], parts[n + 1]) for n in range(0, len(parts), 2)]
        return parts[0]

    def score(i, lane_max):
        start = pl.multiple_of(i * block, block)
        part = jnp.dot(q_row, key_v[:, pl.ds(start, block)], preferred_element_type=F32)
        part = jnp.where(lane_pos + start < row_len, part, -jnp.inf)
        scores[:, pl.ds(start, block)] = part
        return jnp.maximum(lane_max, fold(jnp.maximum, part))

    lane_max = lax.fori_loop(0, seq_len // block, score, jnp.broadcast_to(s_new, (n_heads, 128)))
    row_max = jnp.max(lane_max, axis=1, keepdims=True)

    def weigh(i, state):
        lane_sum, acc = state
        start = pl.multiple_of(i * block, block)
        weights = jnp.exp2((scores[:, pl.ds(start, block)] - row_max) * scale)
        acc = acc + dot_nt(weights.astype(BF16), value_v[:, pl.ds(start, block)])
        return lane_sum + fold(jnp.add, weights), acc

    first = jnp.exp2((s_new - row_max) * scale)
    state = (jnp.zeros((n_heads, 128), F32), first.astype(BF16).astype(F32) * value_row)
    lane_sum, acc = lax.fori_loop(0, seq_len // block, weigh, state)
    run_sum = first + jnp.sum(lane_sum, axis=1, keepdims=True)
    ctx = acc / run_sum
    ctx_send[...] = jnp.concatenate([ctx[:n_chip], ctx[n_chip:]], axis=1).astype(BF16)

    row = me % n_chip

    def heads_of(c):
        return pl.ds(pl.multiple_of((c // plane) * plane, plane), plane)

    def send_ctx(i, carry):
        other = (chip + i) % n_chip
        remote(ctx_send.at[heads_of(other)], ctx_recv.at[row], ctx_sems.at[0], ctx_in.at[row], 2 * other + half).start()
        return carry

    lax.fori_loop(1, n_chip, send_ctx, 0)

    @pl.when(core != half)
    def _():
        remote(ctx_send.at[heads_of(chip)], ctx_recv.at[row], ctx_sems.at[1], ctx_in.at[row], 2 * chip + half).start()

    @pl.when(core == half)
    def _():
        ctx_recv[row] = ctx_send[heads_of(chip)]

    fix_block = 1024
    fix_pos = lax.broadcasted_iota(jnp.int32, (1, fix_block), 1)
    key_cols = jnp.concatenate([key_new] * (fix_block // 128), axis=1)
    value_cols = jnp.concatenate([value_new] * (fix_block // 128), axis=1)

    def fix(i, carry):
        start = pl.multiple_of(i * fix_block, fix_block)
        at = pl.ds(start, fix_block)
        hit = jnp.broadcast_to(fix_pos + start == row_len, (head_dim, fix_block))
        key_v[:, at] = jnp.where(hit, key_cols, key_v[:, at])
        value_v[:, at] = jnp.where(hit, value_cols, value_v[:, at])
        return carry

    lax.fori_loop(0, seq_len // fix_block, fix, 0)

    weight_half = wo_c.at[pl.ds(0, plane - 1), 0]
    pltpu.make_async_copy(weight_half, weight_half, wo_sems.at[0]).wait()
    pltpu.make_async_copy(weight_half, weight_half, wo_sems.at[1]).wait()
    partner = 2 * chip + 1 - core
    swap = remote(wo_c.at[:, core], wo_c.at[:, core], wo_sems.at[2], wo_sems.at[3], partner)
    swap.start()

    def widen(r):
        ctx_wide[pl.ds(pl.multiple_of(r * plane, plane), plane)] = ctx_recv[r].astype(F32)

    def take_ctx(i, carry):
        r = (me + n_dev - i) % n_chip

        @pl.when((core != half) | (i != 0))
        def _():
            pltpu.make_async_copy(ctx_recv.at[r], ctx_recv.at[r], ctx_in.at[r]).wait()

        widen(r)
        return carry

    lax.fori_loop(0, n_chip, take_ctx, 0)
    for h in range(plane):
        ctx_all[:, h * 128:(h + 1) * 128] = ctx_wide[pl.ds(h, half_rows, stride=plane), :].astype(BF16)

    swap.wait()
    k_chips = 4
    total = jnp.zeros((half_rows, wide_cols), F32)
    for n in range(0, plane, k_chips):
        rhs = wo_c[n:n + k_chips].reshape(k_chips * 128, wide_cols)
        total = total + jnp.dot(ctx_all[:, n * 128:(n + k_chips) * 128], rhs, preferred_element_type=F32)
    for j in range(n_grp):
        part = total[:, j * cols:(j + 1) * cols]
        part_own[j % 2, j // 2] = part
        part_send[j % 2, j // 2] = part.astype(BF16)
    parity = group % 2
    for i in (2, 1, 3):
        target = (group + i) % n_grp
        remote(part_send.at[target % 2], part_recv.at[group], part_sems.at[0], part_sems.at[1], 2 * (target * plane + spot) + core).start()
    my_rows = pl.ds(pl.multiple_of(core * half_rows, half_rows), half_rows)
    other_rows = pl.ds(pl.multiple_of((1 - core) * half_rows, half_rows), half_rows)

    def col_block(q, j):
        return pl.ds(pl.multiple_of((q * n_grp + j) * cols, cols), cols)

    part_all = part_recv.at[pl.ds(0, n_grp - 1)]
    pltpu.make_async_copy(part_all, part_all, part_sems.at[1]).wait()
    for n in range(2):
        own = part_own[parity, n] + x_v[my_rows, col_block(spot, parity + 2 * n)].astype(F32)
        for i in range(1, n_grp):
            own = own + part_recv[(group + i) % n_grp, n].astype(F32)
        out_send[n] = own.astype(BF16)

    line = (2 * move(chip, plane, 1) + core, 2 * move(chip, plane, SIDE - 1) + core)
    mine = group // 2

    def pass_line(piece, q):
        for n in range(2):
            remote(piece, out_recv.at[core, q, parity, mine], out_sems.at[1], line_in.at[q, 1 - n], line[n]).start()

    for dy, dx in PLANE_ORDER:
        other = move(move(spot, SIDE, dy), 1, dx)
        remote(out_send, out_recv.at[core, spot, parity], out_sems.at[0], plane_in.at[spot], 2 * (group * plane + other) + core).start()
    pass_line(out_send.at[mine], spot)
    remote(out_send, out_recv.at[core, spot, parity], out_sems.at[2], out_sems.at[3], partner).start()

    def place(q, j, block):
        out_ref[my_rows, col_block(q, j)] = block

    for n in range(2):
        place(spot, parity + 2 * n, out_send[n])

    def receive(piece, sem):
        pltpu.make_async_copy(piece, piece, sem).wait()
        return piece

    for dy, dx in PLANE_ORDER:
        q = move(move(spot, SIDE, SIDE - dy), 1, SIDE - dx)
        pair = receive(out_recv.at[core, q, parity], plane_in.at[q])
        pass_line(pair.at[mine], q)
        remote(pair, pair, out_sems.at[2], out_sems.at[3], partner).start()
        for n in range(2):
            place(q, parity + 2 * n, out_recv[core, q, parity, n])

    for dy, dx in ((0, 0),) + PLANE_ORDER:
        q = move(move(spot, SIDE, SIDE - dy), 1, SIDE - dx)
        for n in range(2):
            j = (group + 1 + 2 * n) % n_grp
            piece = receive(out_recv.at[core, q, 1 - parity, j // 2], line_in.at[q, n])
            remote(piece, piece, out_sems.at[2], out_sems.at[3], partner).start()
            place(q, j, out_recv[core, q, 1 - parity, j // 2])

    ctx_part = ctx_recv.at[pl.ds(0, n_chip - 1)]
    pltpu.make_async_copy(ctx_part, ctx_part, ctx_sems.at[0]).wait()

    @pl.when(core != half)
    def _():
        pltpu.make_async_copy(ctx_recv.at[0], ctx_recv.at[0], ctx_sems.at[1]).wait()

    pltpu.make_async_copy(part_all, part_all, part_sems.at[0]).wait()
    sent = out_recv.at[0, pl.ds(0, plane - 1), 0]
    pltpu.make_async_copy(sent, sent, out_sems.at[0]).wait()
    pltpu.make_async_copy(out_recv.at[0, :, 0], out_recv.at[0, :, 0], out_sems.at[1]).wait()
    pltpu.make_async_copy(out_recv.at[0], out_recv.at[0], out_sems.at[2]).wait()
    pltpu.make_async_copy(out_recv.at[1], out_recv.at[1], out_sems.at[3]).wait()
    for q in range(plane):
        for j in range(n_grp):
            out_ref[other_rows, (q * n_grp + j) * cols:(q * n_grp + j + 1) * cols] = out_recv[1 - core, q, j % 2, j // 2]


def step(x, wq_t, wk_t, wv_t, wo, key_t, value_t, lengths, n_dev, n_grp):
    n_rows, model_dim = x.shape
    head_dim, seq_len = key_t.shape
    n_chip = n_dev // 2
    cols = model_dim // n_chip
    plane = n_chip // n_grp
    dma = pltpu.SemaphoreType.DMA
    return pl.pallas_call(
        functools.partial(step_kernel, n_dev, n_grp),
        out_shape=(pltpu.VMEM(x.shape, BF16), pltpu.VMEM(key_t.shape, BF16), pltpu.VMEM(value_t.shape, BF16)),
        in_specs=[pl.BlockSpec(memory_space=pltpu.HBM)] * 7 + [pl.BlockSpec(memory_space=pltpu.SMEM)],
        out_specs=(pl.BlockSpec(memory_space=pltpu.VMEM),) * 3,
        scratch_shapes=[
            pltpu.VMEM(x.shape, BF16), pltpu.VMEM(wq_t.shape, BF16), pltpu.VMEM(wk_t.shape, BF16), pltpu.VMEM(wv_t.shape, BF16),
            pltpu.VMEM(wo.shape, BF16),
            pltpu.VMEM((n_dev, 1, 128), F32), pltpu.VMEM((n_dev, 1, 128), F32),
            pltpu.VMEM((plane, head_dim, cols * n_grp), BF16),
            pltpu.VMEM((plane, 2, head_dim, cols * n_grp), BF16),
            pltpu.VMEM((n_chip, 128), BF16), pltpu.VMEM((n_chip, plane, 128), BF16), pltpu.VMEM((n_chip * plane, 128), F32),
            pltpu.VMEM((n_rows // 2, plane * 128), BF16),
            pltpu.VMEM((2, 2, n_rows // 2, cols), F32), pltpu.VMEM((2, 2, n_rows // 2, cols), BF16), pltpu.VMEM((n_grp, 2, n_rows // 2, cols), BF16),
            pltpu.VMEM((2, n_rows // 2, cols), BF16),
            pltpu.VMEM((2, plane, 2, 2, n_rows // 2, cols), BF16), pltpu.VMEM((n_dev, seq_len), F32),
            dma((7,)), dma((2,)), dma((4,)), dma((2,)), dma((n_chip,)), dma((2,)), dma((4,)), dma((plane,)), dma((plane, 2)),
        ],
        compiler_params=pltpu.CompilerParams(collective_id=0, has_side_effects=True, vmem_limit_bytes=VMEM_MIB * 1024 * 1024),
        name='decode_step',
    )(x, wq_t, wk_t, wv_t, wo, key_t, value_t, lengths)


def finish_kernel(out_v, key_v, value_v, out_hbm, key_hbm, value_hbm, sems):
    pairs = ((out_v, out_hbm), (key_v, key_hbm), (value_v, value_hbm))
    copies = [pltpu.make_async_copy(src, dst, sems.at[n]) for n, (src, dst) in enumerate(pairs)]
    for copy in copies:
        copy.start()
    for copy in copies:
        copy.wait()


def finish(*arrays):
    return pl.pallas_call(
        finish_kernel,
        out_shape=tuple(jax.ShapeDtypeStruct(a.shape, a.dtype) for a in arrays),
        in_specs=[pl.BlockSpec(memory_space=pltpu.VMEM)] * 3,
        out_specs=(pl.BlockSpec(memory_space=pltpu.HBM),) * 3,
        scratch_shapes=[pltpu.SemaphoreType.DMA((3,))],
        compiler_params=pltpu.CompilerParams(vmem_limit_bytes=FINISH_MIB * 1024 * 1024),
        name='finish',
    )(*arrays)


def solution(mesh):
    n_dev = mesh.shape['model']

    def group_step(hidden, w_query, w_key, w_value, w_out, key_cache, value_cache, lengths):
        key_t = key_cache[0].T
        value_t = value_cache[0].T
        out, key_v, value_v = step(hidden, w_query.T, w_key.T, w_value.T, w_out, key_t, value_t, lengths, n_dev, N_GRP)
        out, key_new, value_new = finish(out, key_v, value_v)
        return out, key_new.T[None], value_new.T[None]

    row_spec = P('replica', None)
    cache_spec = P(('replica', 'model'), None, None)
    return jax.shard_map(group_step, mesh=mesh, in_specs=(row_spec, P(None, 'model'), P(None, None), P(None, None), P('model', None), cache_spec, cache_spec, P('replica')), out_specs=(row_spec, cache_spec, cache_spec), check_vma=False)
```

```python
import functools
import jax
import jax.numpy as jnp
from jax import lax
from jax.experimental import pallas as pl
from jax.experimental.pallas import tpu as pltpu
from jax.sharding import PartitionSpec as P

F32 = jnp.float32
BF16 = jnp.bfloat16
NT = (((1,), (1,)), ((), ()))
LOG2E = 1.4426950408889634
VMEM_MIB = 56
N_GRP = 4
UNROLL = 4
SIDE = 4
PLANE_ORDER = ((2, 2), (2, 3), (3, 2), (2, 1), (1, 2), (2, 0), (0, 2), (3, 1), (1, 3), (3, 3), (1, 1), (3, 0), (0, 3), (1, 0), (0, 1))
FINISH_MIB = 16


def dot_nt(lhs, rhs):
    return lax.dot_general(lhs, rhs, NT, preferred_element_type=F32)


def step_kernel(n_dev, n_grp, x_hbm, wq_hbm, wk_hbm, wv_hbm, wo_hbm, key_hbm, value_hbm, len_ref, out_ref, key_v, value_v,
                x_v, wq_v, wk_v, wv_v, wo_v, q_send, q_recv, wo_send, wo_c, ctx_send, ctx_recv, ctx_wide, ctx_all, part_own, part_send, part_recv, out_send, out_recv, scores,
                load_sem, q_sems, wo_sems, wo_in, ctx_sems, ctx_in, part_sems, out_sems, plane_in, line_in):
    me = lax.axis_index('model')
    core = me % 2
    chip = me // 2
    n_chip = n_dev // 2
    half = me // n_chip
    n_rows, model_dim = x_v.shape
    head_dim, seq_len = key_v.shape
    cols = model_dim // n_chip
    half_rows = n_rows // 2
    plane = n_chip // n_grp
    group = chip // plane
    spot = chip % plane
    wide_cols = cols * n_grp

    parts = []
    for stride, size in ((2 * SIDE * SIDE, SIDE), (2 * SIDE, SIDE), (2, SIDE), (1, 2)):
        at = (me // stride) % size
        parts.append([((at + by) % size) * stride for by in range(size)])

    def device_at(dz, dy, dx, dc):
        return parts[0][dz] + parts[1][dy] + parts[2][dx] + parts[3][dc]

    reach = (0, 1, 2, 1)
    chips = [(dz, dy, dx) for dz in range(SIDE) for dy in range(SIDE) for dx in range(SIDE)]
    chips.sort(key=lambda d: -(reach[d[0]] + reach[d[1]] + reach[d[2]]))
    devices = [device_at(*d, dc) for d in chips for dc in (1, 0)][:-1]

    def move(c, stride, by):
        at = (c // stride) % SIDE
        return c + ((at + by) % SIDE - at) * stride

    def remote(src, dst, send_sem, recv_sem, target):
        return pltpu.make_async_remote_copy(src_ref=src, dst_ref=dst, send_sem=send_sem, recv_sem=recv_sem, device_id={'model': target})

    loads = []
    for n, (src, dst) in enumerate(((x_hbm, x_v), (wq_hbm, wq_v), (wo_hbm, wo_v), (wk_hbm, wk_v), (wv_hbm, wv_v), (key_hbm, key_v), (value_hbm, value_v))):
        copy = pltpu.make_async_copy(src, dst, load_sem.at[n])
        loads.append(copy)
    for copy in loads[:3]:
        copy.start()

    barrier = pltpu.get_barrier_semaphore()

    for target in devices:
        pl.semaphore_signal(barrier, inc=1, device_id={'model': target})

    for copy in loads[3:]:
        copy.start()

    loads[0].wait()
    loads[1].wait()
    k_step = 1024

    def project(i, acc):
        at = pl.ds(pl.multiple_of(i * k_step, k_step), k_step)
        return acc + dot_nt(x_v[:, at], wq_v[:, at])

    query = lax.fori_loop(0, model_dim // k_step, project, jnp.zeros((n_rows, head_dim), F32))
    query = query.astype(BF16).astype(F32)
    q_send[:, 0, :] = jnp.concatenate([query, jnp.zeros_like(query)], axis=1)
    slot = core * n_chip + chip
    q_recv[slot] = q_send[me]
    loads[2].wait()
    for c in range(plane):
        wo_send[c] = wo_v[:, c * wide_cols:(c + 1) * wide_cols]
    pl.semaphore_wait(barrier, n_dev - 1)

    for target in devices:
        remote(q_send.at[target], q_recv.at[slot], q_sems.at[0], q_sems.at[1], target).start()

    for dy, dx in PLANE_ORDER:
        other = move(move(spot, SIDE, dy), 1, dx)
        remote(wo_send.at[other], wo_c.at[spot, core], wo_sems.at[0], wo_in.at[spot], 2 * (group * plane + other) + core).start()
    wo_c[spot, core] = wo_send[spot]

    loads[3].wait()
    loads[4].wait()

    def project_new(i, accs):
        at = pl.ds(pl.multiple_of(i * k_step, k_step), k_step)
        rows = x_v[:, at]
        return accs[0] + dot_nt(wk_v[:, at], rows), accs[1] + dot_nt(wv_v[:, at], rows)

    zero_new = jnp.zeros((head_dim, n_rows), F32)
    key_all, value_all = lax.fori_loop(0, model_dim // k_step, project_new, (zero_new, zero_new))
    lanes = lax.broadcasted_iota(jnp.int32, (head_dim, n_rows), 1)
    key_new = jnp.sum(jnp.where(lanes == me, key_all, 0.0), axis=1, keepdims=True)
    value_new = jnp.sum(jnp.where(lanes == me, value_all, 0.0), axis=1, keepdims=True)
    key_new = jnp.broadcast_to(key_new, (head_dim, 128)).astype(BF16)
    value_new = jnp.broadcast_to(value_new, (head_dim, 128)).astype(BF16)

    loads[5].wait()
    loads[6].wait()
    row_len = len_ref[me]

    fix_block = 1024
    fix_pos = lax.broadcasted_iota(jnp.int32, (1, fix_block), 1)
    key_cols = jnp.concatenate([key_new] * (fix_block // 128), axis=1)
    value_cols = jnp.concatenate([value_new] * (fix_block // 128), axis=1)

    def fix(i, carry):
        start = pl.multiple_of(i * fix_block, fix_block)
        at = pl.ds(start, fix_block)
        hit = jnp.broadcast_to(fix_pos + start == row_len, (head_dim, fix_block))
        key_v[:, at] = jnp.where(hit, key_cols, key_v[:, at])
        value_v[:, at] = jnp.where(hit, value_cols, value_v[:, at])
        return carry

    lax.fori_loop(0, seq_len // fix_block, fix, 0)

    pltpu.make_async_copy(q_recv.at[pl.ds(0, n_dev - 1)], q_recv.at[pl.ds(0, n_dev - 1)], q_sems.at[0]).wait()
    pltpu.make_async_copy(q_recv.at[pl.ds(0, n_dev - 1)], q_recv.at[pl.ds(0, n_dev - 1)], q_sems.at[1]).wait()

    q_row = q_recv[:, 0, :][:, :head_dim].astype(BF16)
    scale = (head_dim ** -0.5) * LOG2E
    block = 2048
    n_heads = q_row.shape[0]
    lane_pos = lax.broadcasted_iota(jnp.int32, (1, block), 1)

    def fold(op, array):
        parts = [array[:, n * 128:(n + 1) * 128] for n in range(array.shape[1] // 128)]
        while len(parts) > 1:
            parts = [op(parts[n], parts[n + 1]) for n in range(0, len(parts), 2)]
        return parts[0]

    def score(i, lane_max):
        start = pl.multiple_of(i * block, block)
        part = jnp.dot(q_row, key_v[:, pl.ds(start, block)], preferred_element_type=F32)
        part = jnp.where(lane_pos + start <= row_len, part, -jnp.inf)
        scores[:, pl.ds(start, block)] = part
        return jnp.maximum(lane_max, fold(jnp.maximum, part))

    lane_max = lax.fori_loop(0, seq_len // block, score, jnp.full((n_heads, 128), -jnp.inf, F32), unroll=UNROLL)
    row_max = jnp.max(lane_max, axis=1, keepdims=True)

    def weigh(i, state):
        lane_sum, acc = state
        start = pl.multiple_of(i * block, block)
        weights = jnp.exp2((scores[:, pl.ds(start, block)] - row_max) * scale)
        acc = acc + dot_nt(weights.astype(BF16), value_v[:, pl.ds(start, block)])
        return lane_sum + fold(jnp.add, weights), acc

    state = (jnp.zeros((n_heads, 128), F32), jnp.zeros((n_heads, head_dim), F32))
    lane_sum, acc = lax.fori_loop(0, seq_len // block, weigh, state, unroll=UNROLL)
    run_sum = jnp.sum(lane_sum, axis=1, keepdims=True)
    ctx = acc / run_sum
    ctx_send[...] = jnp.concatenate([ctx[:n_chip], ctx[n_chip:]], axis=1).astype(BF16)

    row = me % n_chip

    def heads_of(c):
        return pl.ds(pl.multiple_of((c // plane) * plane, plane), plane)

    for dz, dy, dx in chips[:-1]:
        target = device_at(dz, dy, dx, 0) - core + half
        heads = pl.ds(pl.multiple_of((parts[0][dz] // (2 * plane)) * plane, plane), plane)
        remote(ctx_send.at[heads], ctx_recv.at[row], ctx_sems.at[0], ctx_in.at[row], target).start()

    @pl.when(core != half)
    def _():
        remote(ctx_send.at[heads_of(chip)], ctx_recv.at[row], ctx_sems.at[1], ctx_in.at[row], 2 * chip + half).start()

    @pl.when(core == half)
    def _():
        ctx_recv[row] = ctx_send[heads_of(chip)]

    partner = 2 * chip + 1 - core

    def swap(q):
        remote(wo_c.at[q, core], wo_c.at[q, core], wo_sems.at[1], wo_sems.at[2], partner).start()

    swap(spot)
    for dy, dx in PLANE_ORDER:
        q = move(move(spot, SIDE, SIDE - dy), 1, SIDE - dx)
        pltpu.make_async_copy(wo_c.at[q, core], wo_c.at[q, core], wo_in.at[q]).wait()
        swap(q)

    def widen(r):
        ctx_wide[pl.ds(pl.multiple_of(r * plane, plane), plane)] = ctx_recv[r].astype(F32)

    def take_ctx(i, carry):
        r = (me + n_dev - i) % n_chip

        @pl.when((core != half) | (i != 0))
        def _():
            pltpu.make_async_copy(ctx_recv.at[r], ctx_recv.at[r], ctx_in.at[r]).wait()

        widen(r)
        return carry

    lax.fori_loop(0, n_chip, take_ctx, 0, unroll=4)
    for h in range(plane):
        ctx_all[:, h * 128:(h + 1) * 128] = ctx_wide[pl.ds(h, half_rows, stride=plane), :].astype(BF16)

    pltpu.make_async_copy(wo_c.at[:, 0], wo_c.at[:, 0], wo_sems.at[2]).wait()
    k_chips = 4
    total = jnp.zeros((half_rows, wide_cols), F32)
    for n in range(0, plane, k_chips):
        rhs = wo_c[n:n + k_chips].reshape(k_chips * 128, wide_cols)
        total = total + jnp.dot(ctx_all[:, n * 128:(n + k_chips) * 128], rhs, preferred_element_type=F32)
    for j in range(n_grp):
        part = total[:, j * cols:(j + 1) * cols]
        part_own[j % 2, j // 2] = part
        part_send[j % 2, j // 2] = part.astype(BF16)
    parity = group % 2
    for i in (2, 1, 3):
        target = (group + i) % n_grp
        remote(part_send.at[target % 2], part_recv.at[group], part_sems.at[0], part_sems.at[1], 2 * (target * plane + spot) + core).start()
    my_rows = pl.ds(pl.multiple_of(core * half_rows, half_rows), half_rows)
    other_rows = pl.ds(pl.multiple_of((1 - core) * half_rows, half_rows), half_rows)

    def col_block(q, j):
        return pl.ds(pl.multiple_of((q * n_grp + j) * cols, cols), cols)

    part_all = part_recv.at[pl.ds(0, n_grp - 1)]
    pltpu.make_async_copy(part_all, part_all, part_sems.at[1]).wait()
    for n in range(2):
        own = part_own[parity, n] + x_v[my_rows, col_block(spot, parity + 2 * n)].astype(F32)
        for i in range(1, n_grp):
            own = own + part_recv[(group + i) % n_grp, n].astype(F32)
        out_send[n] = own.astype(BF16)

    line = (2 * move(chip, plane, 1) + core, 2 * move(chip, plane, SIDE - 1) + core)
    mine = group // 2

    def pass_line(piece, q):
        for n in range(2):
            remote(piece, out_recv.at[core, q, parity, mine], out_sems.at[1], line_in.at[q, 1 - n], line[n]).start()

    for dy, dx in PLANE_ORDER:
        other = move(move(spot, SIDE, dy), 1, dx)
        remote(out_send, out_recv.at[core, spot, parity], out_sems.at[0], plane_in.at[spot], 2 * (group * plane + other) + core).start()
    pass_line(out_send.at[mine], spot)
    remote(out_send, out_recv.at[core, spot, parity], out_sems.at[2], out_sems.at[3], partner).start()

    def place(q, j, block):
        out_ref[my_rows, col_block(q, j)] = block

    for n in range(2):
        place(spot, parity + 2 * n, out_send[n])

    def receive(piece, sem):
        pltpu.make_async_copy(piece, piece, sem).wait()
        return piece

    for dy, dx in PLANE_ORDER:
        q = move(move(spot, SIDE, SIDE - dy), 1, SIDE - dx)
        pair = receive(out_recv.at[core, q, parity], plane_in.at[q])
        pass_line(pair.at[mine], q)
        remote(pair, pair, out_sems.at[2], out_sems.at[3], partner).start()
        for n in range(2):
            place(q, parity + 2 * n, out_recv[core, q, parity, n])

    for dy, dx in ((0, 0),) + PLANE_ORDER:
        q = move(move(spot, SIDE, SIDE - dy), 1, SIDE - dx)
        for n in range(2):
            j = (group + 1 + 2 * n) % n_grp
            piece = receive(out_recv.at[core, q, 1 - parity, j // 2], line_in.at[q, n])
            remote(piece, piece, out_sems.at[2], out_sems.at[3], partner).start()
            place(q, j, out_recv[core, q, 1 - parity, j // 2])

    sent = wo_c.at[pl.ds(0, plane - 1), 0]
    pltpu.make_async_copy(sent, sent, wo_sems.at[0]).wait()
    pltpu.make_async_copy(wo_c.at[:, 0], wo_c.at[:, 0], wo_sems.at[1]).wait()
    ctx_part = ctx_recv.at[pl.ds(0, n_chip - 1)]
    pltpu.make_async_copy(ctx_part, ctx_part, ctx_sems.at[0]).wait()

    @pl.when(core != half)
    def _():
        pltpu.make_async_copy(ctx_recv.at[0], ctx_recv.at[0], ctx_sems.at[1]).wait()

    pltpu.make_async_copy(part_all, part_all, part_sems.at[0]).wait()
    sent = out_recv.at[0, pl.ds(0, plane - 1), 0]
    pltpu.make_async_copy(sent, sent, out_sems.at[0]).wait()
    pltpu.make_async_copy(out_recv.at[0, :, 0], out_recv.at[0, :, 0], out_sems.at[1]).wait()
    pltpu.make_async_copy(out_recv.at[0], out_recv.at[0], out_sems.at[2]).wait()
    pltpu.make_async_copy(out_recv.at[1], out_recv.at[1], out_sems.at[3]).wait()
    for q in range(plane):
        for j in range(n_grp):
            out_ref[other_rows, (q * n_grp + j) * cols:(q * n_grp + j + 1) * cols] = out_recv[1 - core, q, j % 2, j // 2]


def step(x, wq_t, wk_t, wv_t, wo, key_t, value_t, lengths, n_dev, n_grp):
    n_rows, model_dim = x.shape
    head_dim, seq_len = key_t.shape
    n_chip = n_dev // 2
    cols = model_dim // n_chip
    plane = n_chip // n_grp
    dma = pltpu.SemaphoreType.DMA
    return pl.pallas_call(
        functools.partial(step_kernel, n_dev, n_grp),
        out_shape=(pltpu.VMEM(x.shape, BF16), pltpu.VMEM(key_t.shape, BF16), pltpu.VMEM(value_t.shape, BF16)),
        in_specs=[pl.BlockSpec(memory_space=pltpu.HBM)] * 7 + [pl.BlockSpec(memory_space=pltpu.SMEM)],
        out_specs=(pl.BlockSpec(memory_space=pltpu.VMEM),) * 3,
        scratch_shapes=[
            pltpu.VMEM(x.shape, BF16), pltpu.VMEM(wq_t.shape, BF16), pltpu.VMEM(wk_t.shape, BF16), pltpu.VMEM(wv_t.shape, BF16),
            pltpu.VMEM(wo.shape, BF16),
            pltpu.VMEM((n_dev, 1, 128), F32), pltpu.VMEM((n_dev, 1, 128), F32),
            pltpu.VMEM((plane, head_dim, cols * n_grp), BF16),
            pltpu.VMEM((plane, 2, head_dim, cols * n_grp), BF16),
            pltpu.VMEM((n_chip, 128), BF16), pltpu.VMEM((n_chip, plane, 128), BF16), pltpu.VMEM((n_chip * plane, 128), F32),
            pltpu.VMEM((n_rows // 2, plane * 128), BF16),
            pltpu.VMEM((2, 2, n_rows // 2, cols), F32), pltpu.VMEM((2, 2, n_rows // 2, cols), BF16), pltpu.VMEM((n_grp, 2, n_rows // 2, cols), BF16),
            pltpu.VMEM((2, n_rows // 2, cols), BF16),
            pltpu.VMEM((2, plane, 2, 2, n_rows // 2, cols), BF16), pltpu.VMEM((n_dev, seq_len), F32),
            dma((7,)), dma((2,)), dma((3,)), dma((plane,)), dma((2,)), dma((n_chip,)), dma((2,)), dma((4,)), dma((plane,)), dma((plane, 2)),
        ],
        compiler_params=pltpu.CompilerParams(collective_id=0, has_side_effects=True, vmem_limit_bytes=VMEM_MIB * 1024 * 1024),
        name='decode_step',
    )(x, wq_t, wk_t, wv_t, wo, key_t, value_t, lengths)


def finish_kernel(out_v, key_v, value_v, out_hbm, key_hbm, value_hbm, sems):
    pairs = ((out_v, out_hbm), (key_v, key_hbm), (value_v, value_hbm))
    copies = [pltpu.make_async_copy(src, dst, sems.at[n]) for n, (src, dst) in enumerate(pairs)]
    for copy in copies:
        copy.start()
    for copy in copies:
        copy.wait()


def finish(*arrays):
    return pl.pallas_call(
        finish_kernel,
        out_shape=tuple(jax.ShapeDtypeStruct(a.shape, a.dtype) for a in arrays),
        in_specs=[pl.BlockSpec(memory_space=pltpu.VMEM)] * 3,
        out_specs=(pl.BlockSpec(memory_space=pltpu.HBM),) * 3,
        scratch_shapes=[pltpu.SemaphoreType.DMA((3,))],
        compiler_params=pltpu.CompilerParams(vmem_limit_bytes=FINISH_MIB * 1024 * 1024),
        name='finish',
    )(*arrays)


def solution(mesh):
    n_dev = mesh.shape['model']

    def group_step(hidden, w_query, w_key, w_value, w_out, key_cache, value_cache, lengths):
        key_t = key_cache[0].T
        value_t = value_cache[0].T
        out, key_v, value_v = step(hidden, w_query.T, w_key.T, w_value.T, w_out, key_t, value_t, lengths, n_dev, N_GRP)
        out, key_new, value_new = finish(out, key_v, value_v)
        return out, key_new.T[None], value_new.T[None]

    row_spec = P('replica', None)
    cache_spec = P(('replica', 'model'), None, None)
    return jax.shard_map(group_step, mesh=mesh, in_specs=(row_spec, P(None, 'model'), P(None, None), P(None, None), P('model', None), cache_spec, cache_spec, P('replica')), out_specs=(row_spec, cache_spec, cache_spec), check_vma=False)
```

```python
import functools
import jax
import jax.numpy as jnp
from jax import lax
from jax.experimental import pallas as pl
from jax.experimental.pallas import tpu as pltpu
from jax.sharding import PartitionSpec as P

F32 = jnp.float32
BF16 = jnp.bfloat16
NT = (((1,), (1,)), ((), ()))
LOG2E = 1.4426950408889634
VMEM_MIB = 56
UNROLL = 4
SIDE = 4
PLANE_FAR = ((2, 2), (2, 3), (3, 2), (2, 1), (1, 2), (2, 0), (0, 2), (3, 1), (1, 3), (3, 3), (1, 1), (3, 0), (0, 3), (1, 0), (0, 1))
PLANE_NEAR = PLANE_FAR[::-1]
LINE_FAR = (2, 3, 1)
FINISH_MIB = 16


def dot_nt(lhs, rhs):
    return lax.dot_general(lhs, rhs, NT, preferred_element_type=F32)


def step_kernel(n_dev, x_hbm, wq_hbm, wk_hbm, wv_hbm, wo_hbm, key_hbm, value_hbm, len_ref, out_ref, key_v, value_v,
                x_v, wq_v, wk_v, wv_v, wo_v, q_send, q_recv, wo_send, wo_c, ctx_flat, ctx_send, ctx_recv, part_own, part_send, part_recv, out_send, out_recv, scores,
                load_sem, q_sems, wo_sems, wo_in, ctx_sems, part_sems, out_sems, plane_in, line_in):
    me = lax.axis_index('model')
    core = me % 2
    chip = me // 2
    n_chip = n_dev // 2
    half = me // n_chip
    n_rows, model_dim = x_v.shape
    head_dim, seq_len = key_v.shape
    cols = model_dim // n_chip
    half_rows = n_rows // 2
    plane = SIDE * SIDE
    group = chip // plane
    spot = chip % plane
    along = (spot % SIDE, spot // SIDE)
    band = model_dim // (2 * SIDE)

    parts = []
    for stride, size in ((2 * SIDE * SIDE, SIDE), (2 * SIDE, SIDE), (2, SIDE), (1, 2)):
        at = (me // stride) % size
        parts.append([((at + by) % size) * stride for by in range(size)])

    def device_at(dz, dy, dx, dc):
        return parts[0][dz] + parts[1][dy] + parts[2][dx] + parts[3][dc]

    reach = (0, 1, 2, 1)
    chips = [(dz, dy, dx) for dz in range(SIDE) for dy in range(SIDE) for dx in range(SIDE)]
    chips.sort(key=lambda d: -(reach[d[0]] + reach[d[1]] + reach[d[2]]))
    devices = [device_at(*d, dc) for d in chips for dc in (1, 0)][:-1]

    def move(c, stride, by):
        at = (c // stride) % SIDE
        return c + ((at + by) % SIDE - at) * stride

    def remote(src, dst, send_sem, recv_sem, target):
        return pltpu.make_async_remote_copy(src_ref=src, dst_ref=dst, send_sem=send_sem, recv_sem=recv_sem, device_id={'model': target})

    loads = []
    for n, (src, dst) in enumerate(((x_hbm, x_v), (wq_hbm, wq_v), (wo_hbm, wo_v), (wk_hbm, wk_v), (wv_hbm, wv_v), (key_hbm, key_v), (value_hbm, value_v))):
        copy = pltpu.make_async_copy(src, dst, load_sem.at[n])
        loads.append(copy)
    for copy in loads[:3]:
        copy.start()

    barrier = pltpu.get_barrier_semaphore()

    for target in devices:
        pl.semaphore_signal(barrier, inc=1, device_id={'model': target})

    for copy in loads[3:]:
        copy.start()

    loads[0].wait()
    loads[1].wait()
    k_step = 1024

    def project(i, acc):
        at = pl.ds(pl.multiple_of(i * k_step, k_step), k_step)
        return acc + dot_nt(x_v[:, at], wq_v[:, at])

    query = lax.fori_loop(0, model_dim // k_step, project, jnp.zeros((n_rows, head_dim), F32))
    query = query.astype(BF16).astype(F32)
    q_send[:, 0, :] = jnp.concatenate([query, jnp.zeros_like(query)], axis=1)
    slot = core * n_chip + chip
    q_recv[slot] = q_send[me]
    loads[2].wait()
    for n in range(2 * SIDE):
        wo_send[n // SIDE, n % SIDE] = wo_v[:, n * band:(n + 1) * band]
    pl.semaphore_wait(barrier, n_dev - 1)

    for target in devices:
        remote(q_send.at[target], q_recv.at[slot], q_sems.at[0], q_sems.at[1], target).start()

    for by in LINE_FAR:
        for t, stride in enumerate((1, SIDE)):
            other = move(chip, stride, by)
            remote(wo_send.at[t, other // stride % SIDE], wo_c.at[t, along[t], core], wo_sems.at[0], wo_in.at[t, along[t]], 2 * other + core).start()
    for t in range(2):
        wo_c[t, along[t], core] = wo_send[t, along[t]]

    loads[3].wait()
    loads[4].wait()

    def project_new(i, accs):
        at = pl.ds(pl.multiple_of(i * k_step, k_step), k_step)
        rows = x_v[:, at]
        return accs[0] + dot_nt(wk_v[:, at], rows), accs[1] + dot_nt(wv_v[:, at], rows)

    zero_new = jnp.zeros((head_dim, n_rows), F32)
    key_all, value_all = lax.fori_loop(0, model_dim // k_step, project_new, (zero_new, zero_new))
    lanes = lax.broadcasted_iota(jnp.int32, (head_dim, n_rows), 1)
    key_new = jnp.sum(jnp.where(lanes == me, key_all, 0.0), axis=1, keepdims=True)
    value_new = jnp.sum(jnp.where(lanes == me, value_all, 0.0), axis=1, keepdims=True)
    key_new = jnp.broadcast_to(key_new, (head_dim, 128)).astype(BF16)
    value_new = jnp.broadcast_to(value_new, (head_dim, 128)).astype(BF16)

    loads[5].wait()
    loads[6].wait()
    row_len = len_ref[me]

    fix_block = 1024
    fix_pos = lax.broadcasted_iota(jnp.int32, (1, fix_block), 1)
    key_cols = jnp.concatenate([key_new] * (fix_block // 128), axis=1)
    value_cols = jnp.concatenate([value_new] * (fix_block // 128), axis=1)

    def fix(i, carry):
        start = pl.multiple_of(i * fix_block, fix_block)
        at = pl.ds(start, fix_block)
        hit = jnp.broadcast_to(fix_pos + start == row_len, (head_dim, fix_block))
        key_v[:, at] = jnp.where(hit, key_cols, key_v[:, at])
        value_v[:, at] = jnp.where(hit, value_cols, value_v[:, at])
        return carry

    lax.fori_loop(0, seq_len // fix_block, fix, 0)

    pltpu.make_async_copy(q_recv.at[pl.ds(0, n_dev - 1)], q_recv.at[pl.ds(0, n_dev - 1)], q_sems.at[0]).wait()
    pltpu.make_async_copy(q_recv.at[pl.ds(0, n_dev - 1)], q_recv.at[pl.ds(0, n_dev - 1)], q_sems.at[1]).wait()

    q_row = q_recv[:, 0, :][:, :head_dim].astype(BF16)
    scale = (head_dim ** -0.5) * LOG2E
    block = 2048
    n_heads = q_row.shape[0]
    lane_pos = lax.broadcasted_iota(jnp.int32, (1, block), 1)

    def fold(op, array):
        parts = [array[:, n * 128:(n + 1) * 128] for n in range(array.shape[1] // 128)]
        while len(parts) > 1:
            parts = [op(parts[n], parts[n + 1]) for n in range(0, len(parts), 2)]
        return parts[0]

    def score(i, lane_max):
        start = pl.multiple_of(i * block, block)
        part = jnp.dot(q_row, key_v[:, pl.ds(start, block)], preferred_element_type=F32)
        part = jnp.where(lane_pos + start <= row_len, part, -jnp.inf)
        scores[:, pl.ds(start, block)] = part
        return jnp.maximum(lane_max, fold(jnp.maximum, part))

    lane_max = lax.fori_loop(0, seq_len // block, score, jnp.full((n_heads, 128), -jnp.inf, F32), unroll=UNROLL)
    row_max = jnp.max(lane_max, axis=1, keepdims=True)

    def weigh(i, state):
        lane_sum, acc = state
        start = pl.multiple_of(i * block, block)
        weights = jnp.exp2((scores[:, pl.ds(start, block)] - row_max) * scale)
        acc = acc + dot_nt(weights.astype(BF16), value_v[:, pl.ds(start, block)])
        return lane_sum + fold(jnp.add, weights), acc

    state = (jnp.zeros((n_heads, 128), F32), jnp.zeros((n_heads, head_dim), F32))
    lane_sum, acc = lax.fori_loop(0, seq_len // block, weigh, state, unroll=UNROLL)
    run_sum = jnp.sum(lane_sum, axis=1, keepdims=True)
    ctx = acc / run_sum
    ctx_flat[...] = jnp.concatenate([ctx[:n_chip], ctx[n_chip:]], axis=1).astype(BF16).astype(F32)
    for z in range(SIDE):
        rows_x = [ctx_flat[pl.ds(z * plane + n * SIDE, SIDE), :] for n in range(SIDE)]
        rows_y = [ctx_flat[pl.ds(z * plane + n, SIDE, stride=SIDE), :] for n in range(SIDE)]
        for n in range(plane):
            ctx_send[z * plane + n, :SIDE] = rows_x[n // SIDE]
            ctx_send[z * plane + n, SIDE:] = rows_y[n % SIDE]

    row = pl.ds(pl.multiple_of(me % n_chip * 2 * SIDE, 2 * SIDE), 2 * SIDE)
    for dz, dy, dx in chips[:-1]:
        target = device_at(dz, dy, dx, 0) - core
        remote(ctx_send.at[target // 2], ctx_recv.at[row], ctx_sems.at[0], ctx_sems.at[1], target + half).start()

    @pl.when(core != half)
    def _():
        remote(ctx_send.at[chip], ctx_recv.at[row], ctx_sems.at[0], ctx_sems.at[1], 2 * chip + half).start()

    @pl.when(core == half)
    def _():
        ctx_recv[row, :] = ctx_send[chip]

    partner = 2 * chip + 1 - core

    def swap(t, n):
        remote(wo_c.at[t, n, core], wo_c.at[t, n, core], wo_sems.at[1], wo_sems.at[2], partner).start()

    for t in range(2):
        swap(t, along[t])
    for by in LINE_FAR:
        for t in range(2):
            n = (along[t] + SIDE - by) % SIDE
            pltpu.make_async_copy(wo_c.at[t, n, core], wo_c.at[t, n, core], wo_in.at[t, n]).wait()
            swap(t, n)

    ctx_part = ctx_recv.at[pl.ds(0, (n_chip - 1) * 2 * SIDE)]

    def wait_ctx(sem):
        @pl.when(core != half)
        def _():
            pltpu.make_async_copy(ctx_recv, ctx_recv, sem).wait()

        @pl.when(core == half)
        def _():
            pltpu.make_async_copy(ctx_part, ctx_part, sem).wait()

    wait_ctx(ctx_sems.at[1])
    pltpu.make_async_copy(wo_c.at[:, :, 0], wo_c.at[:, :, 0], wo_sems.at[2]).wait()
    for t in range(2):
        lhs = jnp.concatenate([ctx_recv[pl.ds(t * SIDE + h, half_rows, stride=2 * SIDE), :] for h in range(SIDE)], axis=1).astype(BF16)
        for n in range(2):
            rhs = wo_c[t, :, :, :, n * (band // 2):(n + 1) * (band // 2)].reshape(SIDE * 128, band // 2)
            total = jnp.dot(lhs, rhs, preferred_element_type=F32)
            for b in range(SIDE):
                part = total[:, b * cols:(b + 1) * cols]
                part_own[t, n * SIDE + b] = part
                part_send[t, n * SIDE + b] = part.astype(BF16)
    parity = group % 2
    for k, (dz, da) in enumerate(PLANE_FAR):
        for t, stride in enumerate((SIDE, 1)):
            other = move(move(chip, plane, dz), stride, da)
            block_no = other // stride % SIDE * 2 + other // plane % 2
            remote(part_send.at[t, block_no], part_recv.at[t, k], part_sems.at[0], part_sems.at[1], 2 * other + core).start()
    my_rows = pl.ds(pl.multiple_of(core * half_rows, half_rows), half_rows)
    other_rows = pl.ds(pl.multiple_of((1 - core) * half_rows, half_rows), half_rows)

    def col_number(q, par, t):
        x_at, y_at = q % SIDE, q // SIDE
        return (x_at * 2 * SIDE + y_at * 2 if t == 0 else (SIDE + y_at) * 2 * SIDE + x_at * 2) + par

    def col_block(q, par, t):
        return pl.ds(pl.multiple_of(col_number(q, par, t) * cols, cols), cols)

    owns = [part_own[t, along[1 - t] * 2 + parity] + x_v[my_rows, col_block(spot, parity, t)].astype(F32) for t in range(2)]
    pltpu.make_async_copy(part_recv, part_recv, part_sems.at[1]).wait()
    for t in range(2):
        own = owns[t]
        for k in range(len(PLANE_FAR)):
            own = own + part_recv[t, k].astype(F32)
        out_send[t] = own.astype(BF16)

    line = (2 * move(chip, plane, SIDE - 1) + core, 2 * move(chip, plane, 1) + core)

    def pass_line(pair, q):
        for t in range(2):
            remote(pair.at[t], out_recv.at[core, q, parity, t], out_sems.at[1], line_in.at[q, t], line[t]).start()

    for dy, dx in PLANE_NEAR:
        other = move(move(spot, SIDE, dy), 1, dx)
        remote(out_send, out_recv.at[core, spot, parity], out_sems.at[0], plane_in.at[spot], 2 * (group * plane + other) + core).start()
    pass_line(out_send, spot)
    remote(out_send, out_recv.at[core, spot, parity], out_sems.at[2], out_sems.at[3], partner).start()
    for t in range(2):
        out_ref[my_rows, col_block(spot, parity, t)] = out_send[t]

    def receive(piece, sem):
        pltpu.make_async_copy(piece, piece, sem).wait()
        return piece

    for dy, dx in PLANE_NEAR:
        q = move(move(spot, SIDE, SIDE - dy), 1, SIDE - dx)
        pair = receive(out_recv.at[core, q, parity], plane_in.at[q])
        pass_line(pair, q)
        remote(pair, pair, out_sems.at[2], out_sems.at[3], partner).start()
        for t in range(2):
            out_ref[my_rows, col_block(q, parity, t)] = out_recv[core, q, parity, t]

    for dy, dx in ((0, 0),) + PLANE_NEAR:
        q = move(move(spot, SIDE, SIDE - dy), 1, SIDE - dx)
        for t in range(2):
            piece = receive(out_recv.at[core, q, 1 - parity, t], line_in.at[q, t])
            remote(piece, piece, out_sems.at[2], out_sems.at[3], partner).start()
            out_ref[my_rows, col_block(q, 1 - parity, t)] = out_recv[core, q, 1 - parity, t]

    sent = wo_c.at[pl.ds(0, 1), pl.ds(0, SIDE - 1)]
    pltpu.make_async_copy(sent, sent, wo_sems.at[0]).wait()
    pltpu.make_async_copy(wo_c.at[:, :, 0], wo_c.at[:, :, 0], wo_sems.at[1]).wait()
    wait_ctx(ctx_sems.at[0])
    pltpu.make_async_copy(part_recv, part_recv, part_sems.at[0]).wait()
    sent = out_recv.at[0, pl.ds(0, plane - 1), 0]
    pltpu.make_async_copy(sent, sent, out_sems.at[0]).wait()
    pltpu.make_async_copy(out_recv.at[0, :, 0], out_recv.at[0, :, 0], out_sems.at[1]).wait()
    pltpu.make_async_copy(out_recv.at[0], out_recv.at[0], out_sems.at[2]).wait()
    pltpu.make_async_copy(out_recv.at[1], out_recv.at[1], out_sems.at[3]).wait()
    for q in range(plane):
        for n in range(4):
            at = col_number(q, n // 2, n % 2) * cols
            out_ref[other_rows, at:at + cols] = out_recv[1 - core, q, n // 2, n % 2]


def step(x, wq_t, wk_t, wv_t, wo, key_t, value_t, lengths, n_dev):
    n_rows, model_dim = x.shape
    head_dim, seq_len = key_t.shape
    n_chip = n_dev // 2
    cols = model_dim // n_chip
    plane = SIDE * SIDE
    half_rows = n_rows // 2
    dma = pltpu.SemaphoreType.DMA
    return pl.pallas_call(
        functools.partial(step_kernel, n_dev),
        out_shape=(pltpu.VMEM(x.shape, BF16), pltpu.VMEM(key_t.shape, BF16), pltpu.VMEM(value_t.shape, BF16)),
        in_specs=[pl.BlockSpec(memory_space=pltpu.HBM)] * 7 + [pl.BlockSpec(memory_space=pltpu.SMEM)],
        out_specs=(pl.BlockSpec(memory_space=pltpu.VMEM),) * 3,
        scratch_shapes=[
            pltpu.VMEM(x.shape, BF16), pltpu.VMEM(wq_t.shape, BF16), pltpu.VMEM(wk_t.shape, BF16), pltpu.VMEM(wv_t.shape, BF16),
            pltpu.VMEM(wo.shape, BF16),
            pltpu.VMEM((n_dev, 1, 128), F32), pltpu.VMEM((n_dev, 1, 128), F32),
            pltpu.VMEM((2, SIDE, head_dim, model_dim // (2 * SIDE)), BF16),
            pltpu.VMEM((2, SIDE, 2, head_dim, model_dim // (2 * SIDE)), BF16),
            pltpu.VMEM((n_chip, 128), F32), pltpu.VMEM((n_chip, 2 * SIDE, 128), F32), pltpu.VMEM((half_rows * 2 * SIDE, 128), F32),
            pltpu.VMEM((2, 2 * SIDE, half_rows, cols), F32), pltpu.VMEM((2, 2 * SIDE, half_rows, cols), BF16), pltpu.VMEM((2, plane - 1, half_rows, cols), BF16),
            pltpu.VMEM((2, half_rows, cols), BF16),
            pltpu.VMEM((2, plane, 2, 2, n_rows // 2, cols), BF16), pltpu.VMEM((n_dev, seq_len), F32),
            dma((7,)), dma((2,)), dma((3,)), dma((2, SIDE)), dma((2,)), dma((2,)), dma((4,)), dma((plane,)), dma((plane, 2)),
        ],
        compiler_params=pltpu.CompilerParams(collective_id=0, has_side_effects=True, vmem_limit_bytes=VMEM_MIB * 1024 * 1024),
        name='decode_step',
    )(x, wq_t, wk_t, wv_t, wo, key_t, value_t, lengths)


def finish_kernel(out_v, key_v, value_v, out_hbm, key_hbm, value_hbm, sems):
    pairs = ((out_v, out_hbm), (key_v, key_hbm), (value_v, value_hbm))
    copies = [pltpu.make_async_copy(src, dst, sems.at[n]) for n, (src, dst) in enumerate(pairs)]
    for copy in copies:
        copy.start()
    for copy in copies:
        copy.wait()


def finish(*arrays):
    return pl.pallas_call(
        finish_kernel,
        out_shape=tuple(jax.ShapeDtypeStruct(a.shape, a.dtype) for a in arrays),
        in_specs=[pl.BlockSpec(memory_space=pltpu.VMEM)] * 3,
        out_specs=(pl.BlockSpec(memory_space=pltpu.HBM),) * 3,
        scratch_shapes=[pltpu.SemaphoreType.DMA((3,))],
        compiler_params=pltpu.CompilerParams(vmem_limit_bytes=FINISH_MIB * 1024 * 1024),
        name='finish',
    )(*arrays)


def solution(mesh):
    n_dev = mesh.shape['model']

    def group_step(hidden, w_query, w_key, w_value, w_out, key_cache, value_cache, lengths):
        key_t = key_cache[0].T
        value_t = value_cache[0].T
        out, key_v, value_v = step(hidden, w_query.T, w_key.T, w_value.T, w_out, key_t, value_t, lengths, n_dev)
        out, key_new, value_new = finish(out, key_v, value_v)
        return out, key_new.T[None], value_new.T[None]

    row_spec = P('replica', None)
    cache_spec = P(('replica', 'model'), None, None)
    return jax.shard_map(group_step, mesh=mesh, in_specs=(row_spec, P(None, 'model'), P(None, None), P(None, None), P('model', None), cache_spec, cache_spec, P('replica')), out_specs=(row_spec, cache_spec, cache_spec), check_vma=False)
```

```python
import functools
import jax
import jax.numpy as jnp
from jax import lax
from jax.experimental import pallas as pl
from jax.experimental.pallas import tpu as pltpu
from jax.sharding import PartitionSpec as P

F32 = jnp.float32
BF16 = jnp.bfloat16
NT = (((1,), (1,)), ((), ()))
LOG2E = 1.4426950408889634
VMEM_MIB = 56
UNROLL = 4
SIDE = 4
PLANE_FAR = ((2, 2), (2, 3), (3, 2), (2, 1), (1, 2), (2, 0), (0, 2), (3, 1), (1, 3), (3, 3), (1, 1), (3, 0), (0, 3), (1, 0), (0, 1))
PLANE_NEAR = PLANE_FAR[::-1]
LINE_FAR = (2, 3, 1)
RS_ORDER = PLANE_FAR
LAG = 5
FINISH_MIB = 16


def dot_nt(lhs, rhs):
    return lax.dot_general(lhs, rhs, NT, preferred_element_type=F32)


def step_kernel(n_dev, x_hbm, wq_hbm, wk_hbm, wv_hbm, wo_hbm, key_hbm, value_hbm, len_ref, out_ref, key_v, value_v,
                x_v, wq_v, wk_v, wv_v, wo_v, q_send, q_recv, wo_send, wo_c, ctx_flat, ctx_send, ctx_recv, ctx_wide, part_own, part_send, part_recv, out_send, out_recv, scores,
                load_sem, q_sems, wo_sems, wo_in, ctx_sems, part_sems, out_sems, plane_in, line_in):
    me = lax.axis_index('model')
    core = me % 2
    chip = me // 2
    n_chip = n_dev // 2
    half = me // n_chip
    n_rows, model_dim = x_v.shape
    head_dim, seq_len = key_v.shape
    cols = model_dim // n_chip
    half_rows = n_rows // 2
    plane = SIDE * SIDE
    group = chip // plane
    spot = chip % plane
    along = (spot % SIDE, spot // SIDE)
    band = model_dim // (2 * SIDE)

    parts = []
    for stride, size in ((2 * SIDE * SIDE, SIDE), (2 * SIDE, SIDE), (2, SIDE), (1, 2)):
        at = (me // stride) % size
        parts.append([((at + by) % size) * stride for by in range(size)])

    def device_at(dz, dy, dx, dc):
        return parts[0][dz] + parts[1][dy] + parts[2][dx] + parts[3][dc]

    reach = (0, 1, 2, 1)
    chips = [(dz, dy, dx) for dz in range(SIDE) for dy in range(SIDE) for dx in range(SIDE)]
    chips.sort(key=lambda d: -(reach[d[0]] + reach[d[1]] + reach[d[2]]))
    devices = [device_at(*d, dc) for d in chips for dc in (1, 0)][:-1]

    at_z, at_y, at_x = ([(chip // stride + by) % SIDE for by in range(SIDE)] for stride in (SIDE * SIDE, SIDE, 1))

    def move(c, stride, by):
        at = (c // stride) % SIDE
        return c + ((at + by) % SIDE - at) * stride

    def remote(src, dst, send_sem, recv_sem, target):
        return pltpu.make_async_remote_copy(src_ref=src, dst_ref=dst, send_sem=send_sem, recv_sem=recv_sem, device_id={'model': target})

    loads = []
    for n, (src, dst) in enumerate(((x_hbm, x_v), (wq_hbm, wq_v), (wo_hbm, wo_v), (wk_hbm, wk_v), (wv_hbm, wv_v), (key_hbm, key_v), (value_hbm, value_v))):
        copy = pltpu.make_async_copy(src, dst, load_sem.at[n])
        loads.append(copy)
    for copy in loads[:3]:
        copy.start()

    barrier = pltpu.get_barrier_semaphore()

    for target in devices:
        pl.semaphore_signal(barrier, inc=1, device_id={'model': target})

    for copy in loads[3:]:
        copy.start()

    loads[0].wait()
    loads[1].wait()
    k_step = 1024

    def project(i, acc):
        at = pl.ds(pl.multiple_of(i * k_step, k_step), k_step)
        return acc + dot_nt(x_v[:, at], wq_v[:, at])

    query = lax.fori_loop(0, model_dim // k_step, project, jnp.zeros((n_rows, head_dim), F32))
    query = query.astype(BF16).astype(F32)
    q_send[:, 0, :] = jnp.concatenate([query, jnp.zeros_like(query)], axis=1)
    slot = core * n_chip + chip
    q_recv[slot] = q_send[me]
    loads[2].wait()
    for n in range(2 * SIDE):
        wo_send[n // SIDE, n % SIDE] = wo_v[:, n * band:(n + 1) * band]
    pl.semaphore_wait(barrier, n_dev - 1)

    for target in devices:
        remote(q_send.at[target], q_recv.at[slot], q_sems.at[0], q_sems.at[1], target).start()

    for by in LINE_FAR:
        for t, stride in enumerate((1, SIDE)):
            other = move(chip, stride, by)
            remote(wo_send.at[t, other // stride % SIDE], wo_c.at[t, along[t], core], wo_sems.at[0], wo_in.at[t, along[t]], 2 * other + core).start()
    for t in range(2):
        wo_c[t, along[t], core] = wo_send[t, along[t]]

    loads[3].wait()
    loads[4].wait()

    def project_new(i, accs):
        at = pl.ds(pl.multiple_of(i * k_step, k_step), k_step)
        rows = x_v[:, at]
        return accs[0] + dot_nt(wk_v[:, at], rows), accs[1] + dot_nt(wv_v[:, at], rows)

    zero_new = jnp.zeros((head_dim, n_rows), F32)
    key_all, value_all = lax.fori_loop(0, model_dim // k_step, project_new, (zero_new, zero_new))
    lanes = lax.broadcasted_iota(jnp.int32, (head_dim, n_rows), 1)
    key_new = jnp.sum(jnp.where(lanes == me, key_all, 0.0), axis=1, keepdims=True)
    value_new = jnp.sum(jnp.where(lanes == me, value_all, 0.0), axis=1, keepdims=True)
    key_new = jnp.broadcast_to(key_new, (head_dim, 128)).astype(BF16)
    value_new = jnp.broadcast_to(value_new, (head_dim, 128)).astype(BF16)

    loads[5].wait()
    loads[6].wait()
    row_len = len_ref[me]

    fix_block = 1024
    fix_pos = lax.broadcasted_iota(jnp.int32, (1, fix_block), 1)
    key_cols = jnp.concatenate([key_new] * (fix_block // 128), axis=1)
    value_cols = jnp.concatenate([value_new] * (fix_block // 128), axis=1)

    def fix(i, carry):
        start = pl.multiple_of(i * fix_block, fix_block)
        at = pl.ds(start, fix_block)
        hit = jnp.broadcast_to(fix_pos + start == row_len, (head_dim, fix_block))
        key_v[:, at] = jnp.where(hit, key_cols, key_v[:, at])
        value_v[:, at] = jnp.where(hit, value_cols, value_v[:, at])
        return carry

    lax.fori_loop(0, seq_len // fix_block, fix, 0)

    pltpu.make_async_copy(q_recv.at[pl.ds(0, n_dev - 1)], q_recv.at[pl.ds(0, n_dev - 1)], q_sems.at[0]).wait()
    pltpu.make_async_copy(q_recv.at[pl.ds(0, n_dev - 1)], q_recv.at[pl.ds(0, n_dev - 1)], q_sems.at[1]).wait()

    q_row = q_recv[:, 0, :][:, :head_dim].astype(BF16)
    scale = (head_dim ** -0.5) * LOG2E
    block = 2048
    n_heads = q_row.shape[0]
    lane_pos = lax.broadcasted_iota(jnp.int32, (1, block), 1)

    def fold(op, array):
        parts = [array[:, n * 128:(n + 1) * 128] for n in range(array.shape[1] // 128)]
        while len(parts) > 1:
            parts = [op(parts[n], parts[n + 1]) for n in range(0, len(parts), 2)]
        return parts[0]

    def score(i, lane_max):
        start = pl.multiple_of(i * block, block)
        part = jnp.dot(q_row, key_v[:, pl.ds(start, block)], preferred_element_type=F32)
        part = jnp.where(lane_pos + start <= row_len, part, -jnp.inf)
        scores[:, pl.ds(start, block)] = part
        return jnp.maximum(lane_max, fold(jnp.maximum, part))

    lane_max = lax.fori_loop(0, seq_len // block, score, jnp.full((n_heads, 128), -jnp.inf, F32), unroll=UNROLL)
    row_max = jnp.max(lane_max, axis=1, keepdims=True)

    def weigh(i, state):
        lane_sum, acc = state
        start = pl.multiple_of(i * block, block)
        weights = jnp.exp2((scores[:, pl.ds(start, block)] - row_max) * scale)
        acc = acc + dot_nt(weights.astype(BF16), value_v[:, pl.ds(start, block)])
        return lane_sum + fold(jnp.add, weights), acc

    state = (jnp.zeros((n_heads, 128), F32), jnp.zeros((n_heads, head_dim), F32))
    lane_sum, acc = lax.fori_loop(0, seq_len // block, weigh, state, unroll=UNROLL)
    run_sum = jnp.sum(lane_sum, axis=1, keepdims=True)
    ctx = acc / run_sum
    ctx_flat[...] = jnp.concatenate([ctx[:n_chip], ctx[n_chip:]], axis=1).astype(BF16).astype(F32)
    for z in range(SIDE):
        rows_x = [ctx_flat[pl.ds(z * plane + n * SIDE, SIDE), :] for n in range(SIDE)]
        rows_y = [ctx_flat[pl.ds(z * plane + n, SIDE, stride=SIDE), :] for n in range(SIDE)]
        for n in range(plane):
            ctx_send[z * plane + n] = jnp.concatenate([rows_x[n // SIDE], rows_y[n % SIDE]], axis=0).astype(BF16)

    row = me % n_chip
    for dz, dy, dx in chips[:-1]:
        target = device_at(dz, dy, dx, 0) - core
        remote(ctx_send.at[target // 2], ctx_recv.at[row], ctx_sems.at[0], ctx_sems.at[1], target + half).start()

    @pl.when(core != half)
    def _():
        remote(ctx_send.at[chip], ctx_recv.at[row], ctx_sems.at[0], ctx_sems.at[1], 2 * chip + half).start()

    @pl.when(core == half)
    def _():
        ctx_recv[row] = ctx_send[chip]

    partner = 2 * chip + 1 - core

    def swap(t, n):
        remote(wo_c.at[t, n, core], wo_c.at[t, n, core], wo_sems.at[1], wo_sems.at[2], partner).start()

    for t in range(2):
        swap(t, along[t])
    for by in LINE_FAR:
        for t in range(2):
            n = (along[t] + SIDE - by) % SIDE
            pltpu.make_async_copy(wo_c.at[t, n, core], wo_c.at[t, n, core], wo_in.at[t, n]).wait()
            swap(t, n)

    ctx_part = ctx_recv.at[pl.ds(0, n_chip - 1)]

    def wait_ctx(sem):
        @pl.when(core != half)
        def _():
            pltpu.make_async_copy(ctx_recv, ctx_recv, sem).wait()

        @pl.when(core == half)
        def _():
            pltpu.make_async_copy(ctx_part, ctx_part, sem).wait()

    wait_ctx(ctx_sems.at[1])
    pltpu.make_async_copy(wo_c.at[:, :, 0], wo_c.at[:, :, 0], wo_sems.at[2]).wait()
    for r in range(n_chip):
        ctx_wide[r * 2 * SIDE:(r + 1) * 2 * SIDE] = ctx_recv[r].astype(F32)
    for t in range(2):
        lhs = jnp.concatenate([ctx_wide[pl.ds(t * SIDE + h, half_rows, stride=2 * SIDE), :] for h in range(SIDE)], axis=1).astype(BF16)
        for n in range(2):
            rhs = wo_c[t, :, :, :, n * (band // 2):(n + 1) * (band // 2)].reshape(SIDE * 128, band // 2)
            total = jnp.dot(lhs, rhs, preferred_element_type=F32)
            for b in range(SIDE):
                part = total[:, b * cols:(b + 1) * cols]
                part_own[t, n * SIDE + b] = part
                part_send[t, n * SIDE + b] = part.astype(BF16)
        for k, (dz, da) in enumerate(RS_ORDER):
            side = (at_y, at_x)[t][da]
            other = at_z[dz] * plane + (side * SIDE + at_x[0] if t == 0 else at_y[0] * SIDE + side)
            remote(part_send.at[t, side * 2 + at_z[dz] % 2], part_recv.at[t, k], part_sems.at[0], part_sems.at[1 + t], 2 * other + core).start()

    parity = group % 2
    my_rows = pl.ds(pl.multiple_of(core * half_rows, half_rows), half_rows)
    other_rows = pl.ds(pl.multiple_of((1 - core) * half_rows, half_rows), half_rows)

    def col_number(q, par, t):
        x_at, y_at = q % SIDE, q // SIDE
        return (x_at * 2 * SIDE + y_at * 2 if t == 0 else (SIDE + y_at) * 2 * SIDE + x_at * 2) + par

    def col_block(q, par, t):
        return pl.ds(pl.multiple_of(col_number(q, par, t) * cols, cols), cols)

    line = [2 * (at_z[by] * plane + spot) + core for by in (SIDE - 1, 1)]

    def pass_line(piece, q, t):
        remote(piece, out_recv.at[core, q, parity, t], out_sems.at[1], line_in.at[t, q], line[t]).start()

    def keep(piece, q, par, t):
        remote(piece, out_recv.at[core, q, par, t], out_sems.at[2], out_sems.at[3], partner).start()
        out_ref[my_rows, col_block(q, par, t)] = piece[...]

    for t in range(2):
        own = part_own[t, along[1 - t] * 2 + parity] + x_v[my_rows, col_block(spot, parity, t)].astype(F32)
        pltpu.make_async_copy(part_recv.at[t], part_recv.at[t], part_sems.at[1 + t]).wait()
        for k in range(len(RS_ORDER)):
            own = own + part_recv[t, k].astype(F32)
        out_send[t] = own.astype(BF16)
        for dy, dx in PLANE_NEAR:
            other = group * plane + at_y[dy] * SIDE + at_x[dx]
            remote(out_send.at[t], out_recv.at[core, spot, parity, t], out_sems.at[0], plane_in.at[t, spot], 2 * other + core).start()
        pass_line(out_send.at[t], spot, t)
        keep(out_send.at[t], spot, parity, t)

    def receive(q, par, t, sem):
        piece = out_recv.at[core, q, par, t]
        pltpu.make_async_copy(piece, piece, sem).wait()
        return piece

    spots = [spot] + [at_y[-dy] * SIDE + at_x[-dx] for dy, dx in PLANE_NEAR]

    def in_turn(count):
        turns = [(n, 0) for n in range(count)] + [(n, 1) for n in range(count)]
        return sorted(turns, key=lambda a: a[0] + a[1] * (LAG + 0.5))

    for n, t in in_turn(plane - 1):
        q = spots[n + 1]
        piece = receive(q, parity, t, plane_in.at[t, q])
        pass_line(piece, q, t)
        keep(piece, q, parity, t)
    for n, t in in_turn(plane):
        q = spots[n]
        keep(receive(q, 1 - parity, t, line_in.at[t, q]), q, 1 - parity, t)

    sent = wo_c.at[pl.ds(0, 1), pl.ds(0, SIDE - 1)]
    pltpu.make_async_copy(sent, sent, wo_sems.at[0]).wait()
    pltpu.make_async_copy(wo_c.at[:, :, 0], wo_c.at[:, :, 0], wo_sems.at[1]).wait()
    wait_ctx(ctx_sems.at[0])
    pltpu.make_async_copy(part_recv, part_recv, part_sems.at[0]).wait()
    sent = out_recv.at[0, pl.ds(0, plane - 1), 0]
    pltpu.make_async_copy(sent, sent, out_sems.at[0]).wait()
    pltpu.make_async_copy(out_recv.at[0, :, 0], out_recv.at[0, :, 0], out_sems.at[1]).wait()
    pltpu.make_async_copy(out_recv.at[0], out_recv.at[0], out_sems.at[2]).wait()
    pltpu.make_async_copy(out_recv.at[1], out_recv.at[1], out_sems.at[3]).wait()
    for q in range(plane):
        for n in range(4):
            at = col_number(q, n // 2, n % 2) * cols
            out_ref[other_rows, at:at + cols] = out_recv[1 - core, q, n // 2, n % 2]


def step(x, wq_t, wk_t, wv_t, wo, key_t, value_t, lengths, n_dev):
    n_rows, model_dim = x.shape
    head_dim, seq_len = key_t.shape
    n_chip = n_dev // 2
    cols = model_dim // n_chip
    plane = SIDE * SIDE
    half_rows = n_rows // 2
    dma = pltpu.SemaphoreType.DMA
    return pl.pallas_call(
        functools.partial(step_kernel, n_dev),
        out_shape=(pltpu.VMEM(x.shape, BF16), pltpu.VMEM(key_t.shape, BF16), pltpu.VMEM(value_t.shape, BF16)),
        in_specs=[pl.BlockSpec(memory_space=pltpu.HBM)] * 7 + [pl.BlockSpec(memory_space=pltpu.SMEM)],
        out_specs=(pl.BlockSpec(memory_space=pltpu.VMEM),) * 3,
        scratch_shapes=[
            pltpu.VMEM(x.shape, BF16), pltpu.VMEM(wq_t.shape, BF16), pltpu.VMEM(wk_t.shape, BF16), pltpu.VMEM(wv_t.shape, BF16),
            pltpu.VMEM(wo.shape, BF16),
            pltpu.VMEM((n_dev, 1, 128), F32), pltpu.VMEM((n_dev, 1, 128), F32),
            pltpu.VMEM((2, SIDE, head_dim, model_dim // (2 * SIDE)), BF16),
            pltpu.VMEM((2, SIDE, 2, head_dim, model_dim // (2 * SIDE)), BF16),
            pltpu.VMEM((n_chip, 128), F32), pltpu.VMEM((n_chip, 2 * SIDE, 128), BF16), pltpu.VMEM((n_chip, 2 * SIDE, 128), BF16), pltpu.VMEM((n_chip * 2 * SIDE, 128), F32),
            pltpu.VMEM((2, 2 * SIDE, half_rows, cols), F32), pltpu.VMEM((2, 2 * SIDE, half_rows, cols), BF16), pltpu.VMEM((2, plane - 1, half_rows, cols), BF16),
            pltpu.VMEM((2, half_rows, cols), BF16),
            pltpu.VMEM((2, plane, 2, 2, n_rows // 2, cols), BF16), pltpu.VMEM((n_dev, seq_len), F32),
            dma((7,)), dma((2,)), dma((3,)), dma((2, SIDE)), dma((2,)), dma((3,)), dma((4,)), dma((2, plane)), dma((2, plane)),
        ],
        compiler_params=pltpu.CompilerParams(collective_id=0, has_side_effects=True, vmem_limit_bytes=VMEM_MIB * 1024 * 1024),
        name='decode_step',
    )(x, wq_t, wk_t, wv_t, wo, key_t, value_t, lengths)


def finish_kernel(out_v, key_v, value_v, out_hbm, key_hbm, value_hbm, sems):
    pairs = ((out_v, out_hbm), (key_v, key_hbm), (value_v, value_hbm))
    copies = [pltpu.make_async_copy(src, dst, sems.at[n]) for n, (src, dst) in enumerate(pairs)]
    for copy in copies:
        copy.start()
    for copy in copies:
        copy.wait()


def finish(*arrays):
    return pl.pallas_call(
        finish_kernel,
        out_shape=tuple(jax.ShapeDtypeStruct(a.shape, a.dtype) for a in arrays),
        in_specs=[pl.BlockSpec(memory_space=pltpu.VMEM)] * 3,
        out_specs=(pl.BlockSpec(memory_space=pltpu.HBM),) * 3,
        scratch_shapes=[pltpu.SemaphoreType.DMA((3,))],
        compiler_params=pltpu.CompilerParams(vmem_limit_bytes=FINISH_MIB * 1024 * 1024),
        name='finish',
    )(*arrays)


def solution(mesh):
    n_dev = mesh.shape['model']

    def group_step(hidden, w_query, w_key, w_value, w_out, key_cache, value_cache, lengths):
        key_t = key_cache[0].T
        value_t = value_cache[0].T
        out, key_v, value_v = step(hidden, w_query.T, w_key.T, w_value.T, w_out, key_t, value_t, lengths, n_dev)
        out, key_new, value_new = finish(out, key_v, value_v)
        return out, key_new.T[None], value_new.T[None]

    row_spec = P('replica', None)
    cache_spec = P(('replica', 'model'), None, None)
    return jax.shard_map(group_step, mesh=mesh, in_specs=(row_spec, P(None, 'model'), P(None, None), P(None, None), P('model', None), cache_spec, cache_spec, P('replica')), out_specs=(row_spec, cache_spec, cache_spec), check_vma=False)
```

```python
import functools
import jax
import jax.numpy as jnp
from jax import lax
from jax.experimental import pallas as pl
from jax.experimental.pallas import tpu as pltpu
from jax.sharding import PartitionSpec as P

F32 = jnp.float32
BF16 = jnp.bfloat16
NT = (((1,), (1,)), ((), ()))
LOG2E = 1.4426950408889634
VMEM_MIB = 56
UNROLL = 4
SIDE = 4
PLANE_FAR = ((2, 2), (2, 3), (3, 2), (2, 1), (1, 2), (2, 0), (0, 2), (3, 1), (1, 3), (3, 3), (1, 1), (3, 0), (0, 3), (1, 0), (0, 1))
PLANE_NEAR = PLANE_FAR[::-1]
LINE_FAR = (2, 3, 1)
LINE_NEAR = (1, 3, 2)
RS_ORDER = PLANE_FAR
FINISH_MIB = 16
PIECES = 1


def dot_nt(lhs, rhs):
    return lax.dot_general(lhs, rhs, NT, preferred_element_type=F32)


def step_kernel(n_dev, x_hbm, wq_hbm, wk_hbm, wv_hbm, wo_hbm, key_hbm, value_hbm, len_ref, out_ref, key_v, value_v,
                x_v, wq_v, wk_v, wv_v, wo_v, q_send, q_recv, wo_send, wo_c, ctx_flat, ctx_send, ctx_recv, ctx_wide, part_own, part_send, part_recv, out_send, out_recv, scores,
                load_sem, q_sems, wo_sems, wo_in, ctx_sems, part_sems, out_sems, plane_in, line_in):
    me = lax.axis_index('model')
    core = me % 2
    chip = me // 2
    n_chip = n_dev // 2
    half = me // n_chip
    n_rows, model_dim = x_v.shape
    head_dim, seq_len = key_v.shape
    cols = model_dim // n_chip
    half_rows = n_rows // 2
    plane = SIDE * SIDE
    group = chip // plane
    spot = chip % plane
    along = (spot % SIDE, spot // SIDE)
    band = model_dim // (2 * SIDE)

    parts = []
    for stride, size in ((2 * SIDE * SIDE, SIDE), (2 * SIDE, SIDE), (2, SIDE), (1, 2)):
        at = (me // stride) % size
        parts.append([((at + by) % size) * stride for by in range(size)])

    def device_at(dz, dy, dx, dc):
        return parts[0][dz] + parts[1][dy] + parts[2][dx] + parts[3][dc]

    reach = (0, 1, 2, 1)
    chips = [(dz, dy, dx) for dz in range(SIDE) for dy in range(SIDE) for dx in range(SIDE)]
    chips.sort(key=lambda d: -(reach[d[0]] + reach[d[1]] + reach[d[2]]))
    devices = [device_at(*d, dc) for d in chips for dc in (1, 0)][:-1]

    at_z, at_y, at_x = ([(chip // stride + by) % SIDE for by in range(SIDE)] for stride in (SIDE * SIDE, SIDE, 1))

    def move(c, stride, by):
        at = (c // stride) % SIDE
        return c + ((at + by) % SIDE - at) * stride

    def remote(src, dst, send_sem, recv_sem, target):
        return pltpu.make_async_remote_copy(src_ref=src, dst_ref=dst, send_sem=send_sem, recv_sem=recv_sem, device_id={'model': target})

    loads = []
    for n, (src, dst) in enumerate(((x_hbm, x_v), (wq_hbm, wq_v), (wo_hbm, wo_v), (wk_hbm, wk_v), (wv_hbm, wv_v), (key_hbm, key_v), (value_hbm, value_v))):
        copy = pltpu.make_async_copy(src, dst, load_sem.at[n])
        loads.append(copy)
    for copy in loads[:3]:
        copy.start()

    barrier = pltpu.get_barrier_semaphore()

    for target in devices:
        pl.semaphore_signal(barrier, inc=1, device_id={'model': target})

    for copy in loads[3:]:
        copy.start()

    loads[0].wait()
    loads[1].wait()
    k_step = 1024

    def project(i, acc):
        at = pl.ds(pl.multiple_of(i * k_step, k_step), k_step)
        return acc + dot_nt(x_v[:, at], wq_v[:, at])

    query = lax.fori_loop(0, model_dim // k_step, project, jnp.zeros((n_rows, head_dim), F32))
    query = query.astype(BF16).astype(F32)
    q_send[:, 0, :] = jnp.concatenate([query, jnp.zeros_like(query)], axis=1)
    slot = core * n_chip + chip
    q_recv[slot] = q_send[me]
    loads[2].wait()
    for n in range(2 * SIDE):
        wo_send[n // SIDE, n % SIDE] = wo_v[:, n * band:(n + 1) * band]
    pl.semaphore_wait(barrier, n_dev - 1)

    for target in devices:
        remote(q_send.at[target], q_recv.at[slot], q_sems.at[0], q_sems.at[1], target).start()

    loads[3].wait()
    loads[4].wait()

    def project_new(i, accs):
        at = pl.ds(pl.multiple_of(i * k_step, k_step), k_step)
        rows = x_v[:, at]
        return accs[0] + dot_nt(wk_v[:, at], rows), accs[1] + dot_nt(wv_v[:, at], rows)

    zero_new = jnp.zeros((head_dim, n_rows), F32)
    key_all, value_all = lax.fori_loop(0, model_dim // k_step, project_new, (zero_new, zero_new))
    lanes = lax.broadcasted_iota(jnp.int32, (head_dim, n_rows), 1)
    key_new = jnp.sum(jnp.where(lanes == me, key_all, 0.0), axis=1, keepdims=True)
    value_new = jnp.sum(jnp.where(lanes == me, value_all, 0.0), axis=1, keepdims=True)
    key_new = jnp.broadcast_to(key_new, (head_dim, 128)).astype(BF16)
    value_new = jnp.broadcast_to(value_new, (head_dim, 128)).astype(BF16)

    for by in LINE_FAR:
        for t, stride in enumerate((1, SIDE)):
            other = move(chip, stride, by)
            remote(wo_send.at[t, other // stride % SIDE], wo_c.at[t, along[t], core], wo_sems.at[0], wo_in.at[t, along[t]], 2 * other + core).start()
    for t in range(2):
        wo_c[t, along[t], core] = wo_send[t, along[t]]

    loads[5].wait()
    loads[6].wait()
    row_len = len_ref[me]

    fix_block = 1024
    fix_pos = lax.broadcasted_iota(jnp.int32, (1, fix_block), 1)
    key_cols = jnp.concatenate([key_new] * (fix_block // 128), axis=1)
    value_cols = jnp.concatenate([value_new] * (fix_block // 128), axis=1)

    def fix(i, carry):
        start = pl.multiple_of(i * fix_block, fix_block)
        at = pl.ds(start, fix_block)
        hit = jnp.broadcast_to(fix_pos + start == row_len, (head_dim, fix_block))
        key_v[:, at] = jnp.where(hit, key_cols, key_v[:, at])
        value_v[:, at] = jnp.where(hit, value_cols, value_v[:, at])
        return carry

    lax.fori_loop(0, seq_len // fix_block, fix, 0)

    pltpu.make_async_copy(q_recv.at[pl.ds(0, n_dev - 1)], q_recv.at[pl.ds(0, n_dev - 1)], q_sems.at[0]).wait()
    pltpu.make_async_copy(q_recv.at[pl.ds(0, n_dev - 1)], q_recv.at[pl.ds(0, n_dev - 1)], q_sems.at[1]).wait()

    q_row = q_recv[:, 0, :][:, :head_dim].astype(BF16)
    scale = (head_dim ** -0.5) * LOG2E
    block = 2048
    n_heads = q_row.shape[0]
    lane_pos = lax.broadcasted_iota(jnp.int32, (1, block), 1)

    def fold(op, array):
        parts = [array[:, n * 128:(n + 1) * 128] for n in range(array.shape[1] // 128)]
        while len(parts) > 1:
            parts = [op(parts[n], parts[n + 1]) for n in range(0, len(parts), 2)]
        return parts[0]

    def score(i, lane_max):
        start = pl.multiple_of(i * block, block)
        part = jnp.dot(q_row, key_v[:, pl.ds(start, block)], preferred_element_type=F32)
        part = jnp.where(lane_pos + start <= row_len, part, -jnp.inf)
        scores[:, pl.ds(start, block)] = part
        return jnp.maximum(lane_max, fold(jnp.maximum, part))

    lane_max = lax.fori_loop(0, seq_len // block, score, jnp.full((n_heads, 128), -jnp.inf, F32), unroll=UNROLL)
    row_max = jnp.max(lane_max, axis=1, keepdims=True)

    def weigh(i, state):
        lane_sum, acc = state
        start = pl.multiple_of(i * block, block)
        weights = jnp.exp2((scores[:, pl.ds(start, block)] - row_max) * scale)
        acc = acc + dot_nt(weights.astype(BF16), value_v[:, pl.ds(start, block)])
        return lane_sum + fold(jnp.add, weights), acc

    state = (jnp.zeros((n_heads, 128), F32), jnp.zeros((n_heads, head_dim), F32))
    lane_sum, acc = lax.fori_loop(0, seq_len // block, weigh, state, unroll=UNROLL)
    run_sum = jnp.sum(lane_sum, axis=1, keepdims=True)
    ctx = acc / run_sum
    ctx_flat[...] = jnp.concatenate([ctx[:n_chip], ctx[n_chip:]], axis=1).astype(BF16).astype(F32)
    for z in range(SIDE):
        rows_x = [ctx_flat[pl.ds(z * plane + n * SIDE, SIDE), :] for n in range(SIDE)]
        rows_y = [ctx_flat[pl.ds(z * plane + n, SIDE, stride=SIDE), :] for n in range(SIDE)]
        for n in range(plane):
            ctx_send[z * plane + n] = jnp.concatenate([rows_x[n // SIDE], rows_y[n % SIDE]], axis=0).astype(BF16)

    row = me % n_chip
    for dz, dy, dx in chips[:-1]:
        target = device_at(dz, dy, dx, 0) - core
        remote(ctx_send.at[target // 2], ctx_recv.at[row], ctx_sems.at[0], ctx_sems.at[1], target + half).start()

    @pl.when(core != half)
    def _():
        remote(ctx_send.at[chip], ctx_recv.at[row], ctx_sems.at[0], ctx_sems.at[1], 2 * chip + half).start()

    @pl.when(core == half)
    def _():
        ctx_recv[row] = ctx_send[chip]

    partner = 2 * chip + 1 - core

    def swap(t, n):
        remote(wo_c.at[t, n, core], wo_c.at[t, n, core], wo_sems.at[1], wo_sems.at[2], partner).start()

    for t in range(2):
        swap(t, along[t])
    for by in LINE_FAR:
        for t in range(2):
            n = (along[t] + SIDE - by) % SIDE
            pltpu.make_async_copy(wo_c.at[t, n, core], wo_c.at[t, n, core], wo_in.at[t, n]).wait()
            swap(t, n)

    ctx_part = ctx_recv.at[pl.ds(0, n_chip - 1)]

    def wait_ctx(sem):
        @pl.when(core != half)
        def _():
            pltpu.make_async_copy(ctx_recv, ctx_recv, sem).wait()

        @pl.when(core == half)
        def _():
            pltpu.make_async_copy(ctx_part, ctx_part, sem).wait()

    wait_ctx(ctx_sems.at[1])
    pltpu.make_async_copy(wo_c.at[:, :, 0], wo_c.at[:, :, 0], wo_sems.at[2]).wait()
    for r in range(n_chip):
        ctx_wide[r * 2 * SIDE:(r + 1) * 2 * SIDE] = ctx_recv[r].astype(F32)
    for t in range(2):
        lhs = jnp.concatenate([ctx_wide[pl.ds(t * SIDE + h, half_rows, stride=2 * SIDE), :] for h in range(SIDE)], axis=1).astype(BF16)
        for n in range(2):
            rhs = wo_c[t, :, :, :, n * (band // 2):(n + 1) * (band // 2)].reshape(SIDE * 128, band // 2)
            total = jnp.dot(lhs, rhs, preferred_element_type=F32)
            for b in range(SIDE):
                part = total[:, b * cols:(b + 1) * cols]
                part_own[t, n * SIDE + b] = part
                part_send[t, n * SIDE + b] = part.astype(BF16)
        for k, (dz, da) in enumerate(RS_ORDER):
            side = (at_y, at_x)[t][da]
            other = at_z[dz] * plane + (side * SIDE + at_x[0] if t == 0 else at_y[0] * SIDE + side)
            remote(part_send.at[t, side * 2 + at_z[dz] % 2], part_recv.at[t, k], part_sems.at[0], part_sems.at[1 + t], 2 * other + core).start()

    parity = group % 2
    my_rows = pl.ds(pl.multiple_of(core * half_rows, half_rows), half_rows)
    other_rows = pl.ds(pl.multiple_of((1 - core) * half_rows, half_rows), half_rows)

    def col_number(q, par, t):
        x_at, y_at = q % SIDE, q // SIDE
        return (x_at * 2 * SIDE + y_at * 2 if t == 0 else (SIDE + y_at) * 2 * SIDE + x_at * 2) + par

    def col_block(q, par, t):
        return pl.ds(pl.multiple_of(col_number(q, par, t) * cols, cols), cols)

    line = [2 * (at_z[by] * plane + spot) + core for by in (SIDE - 1, 1)]

    def share(piece, q, t, axis, by):
        other = at_y[0] * SIDE + at_x[by] if axis == 0 else at_y[by] * SIDE + at_x[0]
        remote(piece, out_recv.at[core, q, parity, t], out_sems.at[0], plane_in.at[t, q], 2 * (group * plane + other) + core).start()

    def pass_line(piece, q, t):
        remote(piece, out_recv.at[core, q, parity, t], out_sems.at[1], line_in.at[t, q], line[t]).start()

    def keep(piece, q, par, t):
        remote(piece, out_recv.at[core, q, par, t], out_sems.at[2], out_sems.at[3], partner).start()
        out_ref[my_rows, col_block(q, par, t)] = piece[...]

    for t in range(2):
        own = part_own[t, along[1 - t] * 2 + parity] + x_v[my_rows, col_block(spot, parity, t)].astype(F32)
        pltpu.make_async_copy(part_recv.at[t], part_recv.at[t], part_sems.at[1 + t]).wait()
        for k in range(len(RS_ORDER)):
            own = own + part_recv[t, k].astype(F32)
        out_send[t] = own.astype(BF16)
        for by in LINE_NEAR:
            share(out_send.at[t], spot, t, t, by)
        pass_line(out_send.at[t], spot, t)
        for by in LINE_NEAR:
            share(out_send.at[t], spot, t, 1 - t, by)
        keep(out_send.at[t], spot, parity, t)

    def receive(q, par, t, sem):
        piece = out_recv.at[core, q, par, t]
        pltpu.make_async_copy(piece, piece, sem).wait()
        return piece

    hops = [(first, second) for first in LINE_NEAR for second in LINE_NEAR]
    hops.sort(key=lambda d: reach[d[0]] + reach[d[1]])
    hops = [(0, 0)] + [(by, 0) for by in LINE_NEAR] + [(0, by) for by in LINE_NEAR] + hops

    def spot_at(n, t):
        dx, dy = hops[n] if t == 0 else hops[n][::-1]
        return at_y[-dy] * SIDE + at_x[-dx]

    turns = []
    for n, (first, second) in enumerate(hops):
        for t in range(2):
            late = t + 0.3 * (reach[first] + reach[second])
            if n:
                turns.append((late + (6.0 if first and second else 2.5), 'plane', n, t))
            turns.append((late + (1.5 if n == 0 else 8.5 if second else 5.0), 'line', n, t))
    for _, kind, n, t in sorted(turns):
        q = spot_at(n, t)
        first, second = hops[n]
        if kind == 'plane':
            piece = receive(q, parity, t, plane_in.at[t, q])
            if second == 0:
                for by in LINE_NEAR:
                    share(piece, q, t, 1 - t, by)
            if second != 2:
                pass_line(piece, q, t)
            keep(piece, q, parity, t)
        else:
            piece = receive(q, 1 - parity, t, line_in.at[t, q])
            if second == 0:
                other = at_y[2] * SIDE + at_x[0] if t == 0 else at_y[0] * SIDE + at_x[2]
                remote(piece, piece, out_sems.at[1], line_in.at[t, q], 2 * (group * plane + other) + core).start()
            keep(piece, q, 1 - parity, t)

    sent = wo_c.at[pl.ds(0, 1), pl.ds(0, SIDE - 1)]
    pltpu.make_async_copy(sent, sent, wo_sems.at[0]).wait()
    pltpu.make_async_copy(wo_c.at[:, :, 0], wo_c.at[:, :, 0], wo_sems.at[1]).wait()
    wait_ctx(ctx_sems.at[0])
    pltpu.make_async_copy(part_recv, part_recv, part_sems.at[0]).wait()
    sent = out_recv.at[0, pl.ds(0, plane - 1), 0]
    pltpu.make_async_copy(sent, sent, out_sems.at[0]).wait()
    pltpu.make_async_copy(out_recv.at[0, :, 0], out_recv.at[0, :, 0], out_sems.at[1]).wait()
    pltpu.make_async_copy(out_recv.at[0], out_recv.at[0], out_sems.at[2]).wait()
    pltpu.make_async_copy(out_recv.at[1], out_recv.at[1], out_sems.at[3]).wait()
    for q in range(plane):
        for n in range(4):
            at = col_number(q, n // 2, n % 2) * cols
            out_ref[other_rows, at:at + cols] = out_recv[1 - core, q, n // 2, n % 2]


def step(x, wq_t, wk_t, wv_t, wo, key_t, value_t, lengths, n_dev):
    n_rows, model_dim = x.shape
    head_dim, seq_len = key_t.shape
    n_chip = n_dev // 2
    cols = model_dim // n_chip
    plane = SIDE * SIDE
    half_rows = n_rows // 2
    dma = pltpu.SemaphoreType.DMA
    return pl.pallas_call(
        functools.partial(step_kernel, n_dev),
        out_shape=(pltpu.VMEM(x.shape, BF16), pltpu.VMEM(key_t.shape, BF16), pltpu.VMEM(value_t.shape, BF16)),
        in_specs=[pl.BlockSpec(memory_space=pltpu.HBM)] * 7 + [pl.BlockSpec(memory_space=pltpu.SMEM)],
        out_specs=(pl.BlockSpec(memory_space=pltpu.VMEM),) * 3,
        scratch_shapes=[
            pltpu.VMEM(x.shape, BF16), pltpu.VMEM(wq_t.shape, BF16), pltpu.VMEM(wk_t.shape, BF16), pltpu.VMEM(wv_t.shape, BF16),
            pltpu.VMEM(wo.shape, BF16),
            pltpu.VMEM((n_dev, 1, 128), F32), pltpu.VMEM((n_dev, 1, 128), F32),
            pltpu.VMEM((2, SIDE, head_dim, model_dim // (2 * SIDE)), BF16),
            pltpu.VMEM((2, SIDE, 2, head_dim, model_dim // (2 * SIDE)), BF16),
            pltpu.VMEM((n_chip, 128), F32), pltpu.VMEM((n_chip, 2 * SIDE, 128), BF16), pltpu.VMEM((n_chip, 2 * SIDE, 128), BF16), pltpu.VMEM((n_chip * 2 * SIDE, 128), F32),
            pltpu.VMEM((2, 2 * SIDE, half_rows, cols), F32), pltpu.VMEM((2, 2 * SIDE, half_rows, cols), BF16), pltpu.VMEM((2, plane - 1, half_rows, cols), BF16),
            pltpu.VMEM((2, half_rows, cols), BF16),
            pltpu.VMEM((2, plane, 2, 2, n_rows // 2, cols), BF16), pltpu.VMEM((n_dev, seq_len), F32),
            dma((7,)), dma((2,)), dma((3,)), dma((2, SIDE)), dma((2,)), dma((3,)), dma((4,)), dma((2, plane)), dma((2, plane)),
        ],
        compiler_params=pltpu.CompilerParams(collective_id=0, has_side_effects=True, vmem_limit_bytes=VMEM_MIB * 1024 * 1024),
        name='decode_step',
    )(x, wq_t, wk_t, wv_t, wo, key_t, value_t, lengths)


def finish_kernel(out_v, key_v, value_v, out_hbm, key_hbm, value_hbm, sems):
    copies = []
    for n in range(PIECES):
        for src, dst in ((out_v, out_hbm), (key_v, key_hbm), (value_v, value_hbm)):
            rows = src.shape[0] // PIECES
            at = pl.ds(n * rows, rows)
            copies.append(pltpu.make_async_copy(src.at[at], dst.at[at], sems.at[len(copies)]))
            copies[-1].start()
    for copy in copies:
        copy.wait()


def finish(*arrays):
    return pl.pallas_call(
        finish_kernel,
        out_shape=tuple(jax.ShapeDtypeStruct(a.shape, a.dtype) for a in arrays),
        in_specs=[pl.BlockSpec(memory_space=pltpu.VMEM)] * 3,
        out_specs=(pl.BlockSpec(memory_space=pltpu.HBM),) * 3,
        scratch_shapes=[pltpu.SemaphoreType.DMA((3 * PIECES,))],
        compiler_params=pltpu.CompilerParams(vmem_limit_bytes=FINISH_MIB * 1024 * 1024),
        name='finish',
    )(*arrays)


def solution(mesh):
    n_dev = mesh.shape['model']

    def group_step(hidden, w_query, w_key, w_value, w_out, key_cache, value_cache, lengths):
        key_t = key_cache[0].T
        value_t = value_cache[0].T
        out, key_v, value_v = step(hidden, w_query.T, w_key.T, w_value.T, w_out, key_t, value_t, lengths, n_dev)
        out, key_new, value_new = finish(out, key_v, value_v)
        return out, key_new.T[None], value_new.T[None]

    row_spec = P('replica', None)
    cache_spec = P(('replica', 'model'), None, None)
    return jax.shard_map(group_step, mesh=mesh, in_specs=(row_spec, P(None, 'model'), P(None, None), P(None, None), P('model', None), cache_spec, cache_spec, P('replica')), out_specs=(row_spec, cache_spec, cache_spec), check_vma=False)
```

```python
import functools
import jax
import jax.numpy as jnp
from jax import lax
from jax.experimental import pallas as pl
from jax.experimental.pallas import tpu as pltpu
from jax.sharding import PartitionSpec as P

F32 = jnp.float32
BF16 = jnp.bfloat16
NT = (((1,), (1,)), ((), ()))
LOG2E = 1.4426950408889634
VMEM_MIB = 56
UNROLL = 4
SIDE = 4
PLANE_FAR = ((2, 2), (2, 3), (3, 2), (2, 1), (1, 2), (2, 0), (0, 2), (3, 1), (1, 3), (3, 3), (1, 1), (3, 0), (0, 3), (1, 0), (0, 1))
PLANE_NEAR = PLANE_FAR[::-1]
LINE_FAR = (2, 3, 1)
LINE_NEAR = (1, 3, 2)
RS_ORDER = PLANE_FAR
FINISH_MIB = 16
PIECES = 1


def dot_nt(lhs, rhs):
    return lax.dot_general(lhs, rhs, NT, preferred_element_type=F32)


def step_kernel(n_dev, x_hbm, wq_hbm, wk_hbm, wv_hbm, wo_hbm, key_hbm, value_hbm, len_ref, out_ref, key_v, value_v,
                x_v, wq_v, wk_v, wv_v, wo_v, q_send, q_recv, wo_send, wo_c, ctx_flat, ctx_send, ctx_recv, ctx_wide, part_own, part_send, part_recv, out_send, out_recv, scores,
                load_sem, q_sems, wo_sems, wo_in, ctx_sems, part_sems, out_sems, plane_in, line_in):
    me = lax.axis_index('model')
    core = me % 2
    chip = me // 2
    n_chip = n_dev // 2
    half = me // n_chip
    n_rows, model_dim = x_v.shape
    head_dim, seq_len = key_v.shape
    cols = model_dim // n_chip
    half_rows = n_rows // 2
    plane = SIDE * SIDE
    group = chip // plane
    spot = chip % plane
    along = (spot % SIDE, spot // SIDE)
    band = model_dim // (2 * SIDE)

    parts = []
    for stride, size in ((2 * SIDE * SIDE, SIDE), (2 * SIDE, SIDE), (2, SIDE), (1, 2)):
        at = (me // stride) % size
        parts.append([((at + by) % size) * stride for by in range(size)])

    def device_at(dz, dy, dx, dc):
        return parts[0][dz] + parts[1][dy] + parts[2][dx] + parts[3][dc]

    reach = (0, 1, 2, 1)
    chips = [(dz, dy, dx) for dz in range(SIDE) for dy in range(SIDE) for dx in range(SIDE)]
    chips.sort(key=lambda d: -(reach[d[0]] + reach[d[1]] + reach[d[2]]))
    devices = [device_at(*d, dc) for d in chips for dc in (1, 0)][:-1]

    at_z, at_y, at_x = ([(chip // stride + by) % SIDE for by in range(SIDE)] for stride in (SIDE * SIDE, SIDE, 1))

    def move(c, stride, by):
        at = (c // stride) % SIDE
        return c + ((at + by) % SIDE - at) * stride

    def remote(src, dst, send_sem, recv_sem, target):
        return pltpu.make_async_remote_copy(src_ref=src, dst_ref=dst, send_sem=send_sem, recv_sem=recv_sem, device_id={'model': target})

    loads = []
    for n, (src, dst) in enumerate(((x_hbm, x_v), (wq_hbm, wq_v), (wo_hbm, wo_v), (wk_hbm, wk_v), (wv_hbm, wv_v), (key_hbm, key_v), (value_hbm, value_v))):
        copy = pltpu.make_async_copy(src, dst, load_sem.at[n])
        loads.append(copy)
    for copy in loads[:3]:
        copy.start()

    barrier = pltpu.get_barrier_semaphore()

    for target in devices:
        pl.semaphore_signal(barrier, inc=1, device_id={'model': target})

    for copy in loads[3:]:
        copy.start()

    loads[0].wait()
    loads[1].wait()
    k_step = 1024

    def project(i, acc):
        at = pl.ds(pl.multiple_of(i * k_step, k_step), k_step)
        return acc + dot_nt(x_v[:, at], wq_v[:, at])

    query = lax.fori_loop(0, model_dim // k_step, project, jnp.zeros((n_rows, head_dim), F32))
    query = query.astype(BF16).astype(F32)
    q_send[:, 0, :] = jnp.concatenate([query, jnp.zeros_like(query)], axis=1)
    slot = core * n_chip + chip
    q_recv[slot] = q_send[me]
    loads[2].wait()
    for n in range(2 * SIDE):
        wo_send[n // SIDE, n % SIDE] = wo_v[:, n * band:(n + 1) * band]
    pl.semaphore_wait(barrier, n_dev - 1)

    for target in devices:
        remote(q_send.at[target], q_recv.at[slot], q_sems.at[0], q_sems.at[1], target).start()

    loads[3].wait()
    loads[4].wait()

    def project_new(i, accs):
        at = pl.ds(pl.multiple_of(i * k_step, k_step), k_step)
        rows = x_v[:, at]
        return accs[0] + dot_nt(wk_v[:, at], rows), accs[1] + dot_nt(wv_v[:, at], rows)

    zero_new = jnp.zeros((head_dim, n_rows), F32)
    key_all, value_all = lax.fori_loop(0, model_dim // k_step, project_new, (zero_new, zero_new))
    lanes = lax.broadcasted_iota(jnp.int32, (head_dim, n_rows), 1)
    key_new = jnp.sum(jnp.where(lanes == me, key_all, 0.0), axis=1, keepdims=True)
    value_new = jnp.sum(jnp.where(lanes == me, value_all, 0.0), axis=1, keepdims=True)
    key_new = jnp.broadcast_to(key_new, (head_dim, 128)).astype(BF16)
    value_new = jnp.broadcast_to(value_new, (head_dim, 128)).astype(BF16)

    for by in LINE_FAR:
        for t, stride in enumerate((1, SIDE)):
            other = move(chip, stride, by)
            remote(wo_send.at[t, other // stride % SIDE], wo_c.at[t, along[t], core], wo_sems.at[0], wo_in.at[t, along[t]], 2 * other + core).start()
    for t in range(2):
        wo_c[t, along[t], core] = wo_send[t, along[t]]

    loads[5].wait()
    loads[6].wait()
    row_len = len_ref[me]

    fix_block = 1024
    fix_pos = lax.broadcasted_iota(jnp.int32, (1, fix_block), 1)
    key_cols = jnp.concatenate([key_new] * (fix_block // 128), axis=1)
    value_cols = jnp.concatenate([value_new] * (fix_block // 128), axis=1)

    def fix(i, carry):
        start = pl.multiple_of(i * fix_block, fix_block)
        at = pl.ds(start, fix_block)
        hit = jnp.broadcast_to(fix_pos + start == row_len, (head_dim, fix_block))
        key_v[:, at] = jnp.where(hit, key_cols, key_v[:, at])
        value_v[:, at] = jnp.where(hit, value_cols, value_v[:, at])
        return carry

    lax.fori_loop(0, seq_len // fix_block, fix, 0)

    pltpu.make_async_copy(q_recv.at[pl.ds(0, n_dev - 1)], q_recv.at[pl.ds(0, n_dev - 1)], q_sems.at[0]).wait()
    pltpu.make_async_copy(q_recv.at[pl.ds(0, n_dev - 1)], q_recv.at[pl.ds(0, n_dev - 1)], q_sems.at[1]).wait()

    q_row = q_recv[:, 0, :][:, :head_dim].astype(BF16)
    scale = (head_dim ** -0.5) * LOG2E
    block = 2048
    n_heads = q_row.shape[0]
    lane_pos = lax.broadcasted_iota(jnp.int32, (1, block), 1)

    def fold(op, array):
        parts = [array[:, n * 128:(n + 1) * 128] for n in range(array.shape[1] // 128)]
        while len(parts) > 1:
            parts = [op(parts[n], parts[n + 1]) for n in range(0, len(parts), 2)]
        return parts[0]

    def score(i, lane_max):
        start = pl.multiple_of(i * block, block)
        part = jnp.dot(q_row, key_v[:, pl.ds(start, block)], preferred_element_type=F32)
        part = jnp.where(lane_pos + start <= row_len, part, -jnp.inf)
        scores[:, pl.ds(start, block)] = part
        return jnp.maximum(lane_max, fold(jnp.maximum, part))

    lane_max = lax.fori_loop(0, seq_len // block, score, jnp.full((n_heads, 128), -jnp.inf, F32), unroll=UNROLL)
    row_max = jnp.max(lane_max, axis=1, keepdims=True)

    def weigh(i, state):
        lane_sum, acc = state
        start = pl.multiple_of(i * block, block)
        weights = jnp.exp2((scores[:, pl.ds(start, block)] - row_max) * scale)
        acc = acc + dot_nt(weights.astype(BF16), value_v[:, pl.ds(start, block)])
        return lane_sum + fold(jnp.add, weights), acc

    state = (jnp.zeros((n_heads, 128), F32), jnp.zeros((n_heads, head_dim), F32))
    lane_sum, acc = lax.fori_loop(0, seq_len // block, weigh, state, unroll=UNROLL)
    run_sum = jnp.sum(lane_sum, axis=1, keepdims=True)
    ctx = acc / run_sum
    ctx_flat[...] = jnp.concatenate([ctx[:n_chip], ctx[n_chip:]], axis=1).astype(BF16).astype(F32)
    for z in range(SIDE):
        rows_x = [ctx_flat[pl.ds(z * plane + n * SIDE, SIDE), :] for n in range(SIDE)]
        rows_y = [ctx_flat[pl.ds(z * plane + n, SIDE, stride=SIDE), :] for n in range(SIDE)]
        for n in range(plane):
            ctx_send[z * plane + n] = jnp.concatenate([rows_x[n // SIDE], rows_y[n % SIDE]], axis=0).astype(BF16)

    row = me % n_chip
    for dz, dy, dx in chips[:-1]:
        target = device_at(dz, dy, dx, 0) - core
        remote(ctx_send.at[target // 2], ctx_recv.at[row], ctx_sems.at[0], ctx_sems.at[1], target + half).start()

    @pl.when(core != half)
    def _():
        remote(ctx_send.at[chip], ctx_recv.at[row], ctx_sems.at[0], ctx_sems.at[1], 2 * chip + half).start()

    @pl.when(core == half)
    def _():
        ctx_recv[row] = ctx_send[chip]

    partner = 2 * chip + 1 - core

    def swap(t, n):
        remote(wo_c.at[t, n, core], wo_c.at[t, n, core], wo_sems.at[1], wo_sems.at[2], partner).start()

    for t in range(2):
        swap(t, along[t])
    for by in LINE_FAR:
        for t in range(2):
            n = (along[t] + SIDE - by) % SIDE
            pltpu.make_async_copy(wo_c.at[t, n, core], wo_c.at[t, n, core], wo_in.at[t, n]).wait()
            swap(t, n)

    ctx_part = ctx_recv.at[pl.ds(0, n_chip - 1)]

    def wait_ctx(sem):
        @pl.when(core != half)
        def _():
            pltpu.make_async_copy(ctx_recv, ctx_recv, sem).wait()

        @pl.when(core == half)
        def _():
            pltpu.make_async_copy(ctx_part, ctx_part, sem).wait()

    wait_ctx(ctx_sems.at[1])
    pltpu.make_async_copy(wo_c.at[:, :, 0], wo_c.at[:, :, 0], wo_sems.at[2]).wait()
    for r in range(n_chip):
        ctx_wide[r * 2 * SIDE:(r + 1) * 2 * SIDE] = ctx_recv[r].astype(F32)
    for t in range(2):
        lhs = jnp.concatenate([ctx_wide[pl.ds(t * SIDE + h, half_rows, stride=2 * SIDE), :] for h in range(SIDE)], axis=1).astype(BF16)
        for n in range(2):
            rhs = wo_c[t, :, :, :, n * (band // 2):(n + 1) * (band // 2)].reshape(SIDE * 128, band // 2)
            total = jnp.dot(lhs, rhs, preferred_element_type=F32)
            for b in range(SIDE):
                part = total[:, b * cols:(b + 1) * cols]
                part_own[t, n * SIDE + b] = part
                part_send[t, n * SIDE + b] = part.astype(BF16)
        for k, (dz, da) in enumerate(RS_ORDER):
            side = (at_y, at_x)[t][da]
            other = at_z[dz] * plane + (side * SIDE + at_x[0] if t == 0 else at_y[0] * SIDE + side)
            remote(part_send.at[t, side * 2 + at_z[dz] % 2], part_recv.at[t, k], part_sems.at[0], part_sems.at[1 + t], 2 * other + core).start()

    parity = group % 2
    my_rows = pl.ds(pl.multiple_of(core * half_rows, half_rows), half_rows)
    other_rows = pl.ds(pl.multiple_of((1 - core) * half_rows, half_rows), half_rows)

    def col_number(q, par, t):
        x_at, y_at = q % SIDE, q // SIDE
        return (x_at * 2 * SIDE + y_at * 2 if t == 0 else (SIDE + y_at) * 2 * SIDE + x_at * 2) + par

    def col_block(q, par, t):
        return pl.ds(pl.multiple_of(col_number(q, par, t) * cols, cols), cols)

    line = [2 * (at_z[by] * plane + spot) + core for by in (SIDE - 1, 1)]

    def share(piece, q, t, axis, by):
        other = at_y[0] * SIDE + at_x[by] if axis == 0 else at_y[by] * SIDE + at_x[0]
        remote(piece, out_recv.at[core, q, parity, t], out_sems.at[0], plane_in.at[t, q], 2 * (group * plane + other) + core).start()

    def pass_line(piece, q, t):
        remote(piece, out_recv.at[core, q, parity, t], out_sems.at[1], line_in.at[t, q], line[t]).start()

    kept = []
    n_early = 3 * n_chip // 4

    def keep(piece, q, par, t):
        last = len(kept) >= n_early
        kept.append((q, par, t))
        remote(piece, out_recv.at[core, q, par, t], out_sems.at[2], out_sems.at[4 if last else 3], partner).start()
        out_ref[my_rows, col_block(q, par, t)] = piece[...]

    for t in range(2):
        own = part_own[t, along[1 - t] * 2 + parity] + x_v[my_rows, col_block(spot, parity, t)].astype(F32)
        pltpu.make_async_copy(part_recv.at[t], part_recv.at[t], part_sems.at[1 + t]).wait()
        for k in range(len(RS_ORDER)):
            own = own + part_recv[t, k].astype(F32)
        out_send[t] = own.astype(BF16)
        for by in LINE_NEAR:
            share(out_send.at[t], spot, t, t, by)
        pass_line(out_send.at[t], spot, t)
        for by in LINE_NEAR:
            share(out_send.at[t], spot, t, 1 - t, by)
        keep(out_send.at[t], spot, parity, t)

    def receive(q, par, t, sem):
        piece = out_recv.at[core, q, par, t]
        pltpu.make_async_copy(piece, piece, sem).wait()
        return piece

    hops = [(first, second) for first in LINE_NEAR for second in LINE_NEAR]
    hops.sort(key=lambda d: reach[d[0]] + reach[d[1]])
    hops = [(0, 0)] + [(by, 0) for by in LINE_NEAR] + [(0, by) for by in LINE_NEAR] + hops

    def spot_at(n, t):
        dx, dy = hops[n] if t == 0 else hops[n][::-1]
        return at_y[-dy] * SIDE + at_x[-dx]

    turns = []
    for n, (first, second) in enumerate(hops):
        for t in range(2):
            late = t + 0.3 * (reach[first] + reach[second])
            if n:
                turns.append((late + (6.0 if first and second else 2.5), 'plane', n, t))
            turns.append((late + (1.5 if n == 0 else 8.5 if second else 5.0), 'line', n, t))
    for _, kind, n, t in sorted(turns):
        q = spot_at(n, t)
        first, second = hops[n]
        if kind == 'plane':
            piece = receive(q, parity, t, plane_in.at[t, q])
            if second == 0:
                for by in LINE_NEAR:
                    share(piece, q, t, 1 - t, by)
            if second != 2:
                pass_line(piece, q, t)
            keep(piece, q, parity, t)
        else:
            piece = receive(q, 1 - parity, t, line_in.at[t, q])
            if second == 0:
                other = at_y[2] * SIDE + at_x[0] if t == 0 else at_y[0] * SIDE + at_x[2]
                remote(piece, piece, out_sems.at[1], line_in.at[t, q], 2 * (group * plane + other) + core).start()
            keep(piece, q, 1 - parity, t)

    early = out_recv.at[1, pl.ds(0, 3 * plane // 4)]
    pltpu.make_async_copy(early, early, out_sems.at[3]).wait()
    for q, par, t in kept[:n_early]:
        out_ref[other_rows, col_block(q, par, t)] = out_recv[1 - core, q, par, t]
    sent = wo_c.at[pl.ds(0, 1), pl.ds(0, SIDE - 1)]
    pltpu.make_async_copy(sent, sent, wo_sems.at[0]).wait()
    pltpu.make_async_copy(wo_c.at[:, :, 0], wo_c.at[:, :, 0], wo_sems.at[1]).wait()
    wait_ctx(ctx_sems.at[0])
    pltpu.make_async_copy(part_recv, part_recv, part_sems.at[0]).wait()
    sent = out_recv.at[0, pl.ds(0, plane - 1), 0]
    pltpu.make_async_copy(sent, sent, out_sems.at[0]).wait()
    pltpu.make_async_copy(out_recv.at[0, :, 0], out_recv.at[0, :, 0], out_sems.at[1]).wait()
    pltpu.make_async_copy(out_recv.at[0], out_recv.at[0], out_sems.at[2]).wait()
    last = out_recv.at[1, pl.ds(0, plane // 4)]
    pltpu.make_async_copy(last, last, out_sems.at[4]).wait()
    for q, par, t in kept[n_early:]:
        out_ref[other_rows, col_block(q, par, t)] = out_recv[1 - core, q, par, t]


def step(x, wq_t, wk_t, wv_t, wo, key_t, value_t, lengths, n_dev):
    n_rows, model_dim = x.shape
    head_dim, seq_len = key_t.shape
    n_chip = n_dev // 2
    cols = model_dim // n_chip
    plane = SIDE * SIDE
    half_rows = n_rows // 2
    dma = pltpu.SemaphoreType.DMA
    return pl.pallas_call(
        functools.partial(step_kernel, n_dev),
        out_shape=(pltpu.VMEM(x.shape, BF16), pltpu.VMEM(key_t.shape, BF16), pltpu.VMEM(value_t.shape, BF16)),
        in_specs=[pl.BlockSpec(memory_space=pltpu.HBM)] * 7 + [pl.BlockSpec(memory_space=pltpu.SMEM)],
        out_specs=(pl.BlockSpec(memory_space=pltpu.VMEM),) * 3,
        scratch_shapes=[
            pltpu.VMEM(x.shape, BF16), pltpu.VMEM(wq_t.shape, BF16), pltpu.VMEM(wk_t.shape, BF16), pltpu.VMEM(wv_t.shape, BF16),
            pltpu.VMEM(wo.shape, BF16),
            pltpu.VMEM((n_dev, 1, 128), F32), pltpu.VMEM((n_dev, 1, 128), F32),
            pltpu.VMEM((2, SIDE, head_dim, model_dim // (2 * SIDE)), BF16),
            pltpu.VMEM((2, SIDE, 2, head_dim, model_dim // (2 * SIDE)), BF16),
            pltpu.VMEM((n_chip, 128), F32), pltpu.VMEM((n_chip, 2 * SIDE, 128), BF16), pltpu.VMEM((n_chip, 2 * SIDE, 128), BF16), pltpu.VMEM((n_chip * 2 * SIDE, 128), F32),
            pltpu.VMEM((2, 2 * SIDE, half_rows, cols), F32), pltpu.VMEM((2, 2 * SIDE, half_rows, cols), BF16), pltpu.VMEM((2, plane - 1, half_rows, cols), BF16),
            pltpu.VMEM((2, half_rows, cols), BF16),
            pltpu.VMEM((2, plane, 2, 2, n_rows // 2, cols), BF16), pltpu.VMEM((n_dev, seq_len), F32),
            dma((7,)), dma((2,)), dma((3,)), dma((2, SIDE)), dma((2,)), dma((3,)), dma((5,)), dma((2, plane)), dma((2, plane)),
        ],
        compiler_params=pltpu.CompilerParams(collective_id=0, has_side_effects=True, vmem_limit_bytes=VMEM_MIB * 1024 * 1024),
        name='decode_step',
    )(x, wq_t, wk_t, wv_t, wo, key_t, value_t, lengths)


def finish_kernel(out_v, key_v, value_v, out_hbm, key_hbm, value_hbm, sems):
    copies = []
    for n in range(PIECES):
        for src, dst in ((out_v, out_hbm), (key_v, key_hbm), (value_v, value_hbm)):
            rows = src.shape[0] // PIECES
            at = pl.ds(n * rows, rows)
            copies.append(pltpu.make_async_copy(src.at[at], dst.at[at], sems.at[len(copies)]))
            copies[-1].start()
    for copy in copies:
        copy.wait()


def finish(*arrays):
    return pl.pallas_call(
        finish_kernel,
        out_shape=tuple(jax.ShapeDtypeStruct(a.shape, a.dtype) for a in arrays),
        in_specs=[pl.BlockSpec(memory_space=pltpu.VMEM)] * 3,
        out_specs=(pl.BlockSpec(memory_space=pltpu.HBM),) * 3,
        scratch_shapes=[pltpu.SemaphoreType.DMA((3 * PIECES,))],
        compiler_params=pltpu.CompilerParams(vmem_limit_bytes=FINISH_MIB * 1024 * 1024),
        name='finish',
    )(*arrays)


def solution(mesh):
    n_dev = mesh.shape['model']

    def group_step(hidden, w_query, w_key, w_value, w_out, key_cache, value_cache, lengths):
        key_t = key_cache[0].T
        value_t = value_cache[0].T
        out, key_v, value_v = step(hidden, w_query.T, w_key.T, w_value.T, w_out, key_t, value_t, lengths, n_dev)
        out, key_new, value_new = finish(out, key_v, value_v)
        return out, key_new.T[None], value_new.T[None]

    row_spec = P('replica', None)
    cache_spec = P(('replica', 'model'), None, None)
    return jax.shard_map(group_step, mesh=mesh, in_specs=(row_spec, P(None, 'model'), P(None, None), P(None, None), P('model', None), cache_spec, cache_spec, P('replica')), out_specs=(row_spec, cache_spec, cache_spec), check_vma=False)
```
